32 devices in a mesh: dp: 1, sp: 32 (over x, y, z, core).
Axes of the slice: x: 2, y: 2, z: 4, core: 2. Of those that a mesh axis runs over, the one named last changes fastest.
Arguments:
- x: bfloat16 [4096, 5120], P(('dp', 'sp'))
- gain: bfloat16 [5120], replicated
- wq: bfloat16 [5120, 4096], replicated
- wk: bfloat16 [5120, 1024], replicated
- wv: bfloat16 [5120, 1024], replicated
- wo: bfloat16 [4096, 5120], replicated
Outputs:
- output: bfloat16 [4096, 5120], P(('dp', 'sp'))
All inputs are finite; a program needn't handle non-finite values.
Results may differ from the reference program's by a relative error of at most 0.012.
Values are sent between devices in bfloat16 or wider.
A program may use at most 2 GiB of HBM per device.

```python
import jax
import jax.numpy as jnp
from jax import lax

ROWS = 4096
D = 5120
HEADS = 32
KV_HEADS = 8
HEAD = 128
THETA = 10000


def setup_inputs(seed: int = 0, part: int = 0) -> dict:
    kx, kn, kq, kk, kv, ko = jax.random.split(jax.random.key(seed), 6)

    def weights(key, rows, columns):
        return jax.random.normal(key, (rows, columns), jnp.float32) * rows**-0.5

    drawn = {
        "x": jax.random.normal(jax.random.fold_in(kx, part), (ROWS, D), jnp.float32),
        "gain": 1 + 0.1 * jax.random.normal(kn, (D,), jnp.float32),
        "wq": 2 * weights(kq, D, HEADS * HEAD),
        "wk": 2 * weights(kk, D, KV_HEADS * HEAD),
        "wv": 4 * weights(kv, D, KV_HEADS * HEAD),
        "wo": weights(ko, HEADS * HEAD, D),
    }
    return {k: v.astype(jnp.bfloat16) for k, v in drawn.items()}


def normed(x, gain):
    wide = x.astype(jnp.float32)
    scale = lax.rsqrt(jnp.mean(wide * wide, -1, keepdims=True) + 1e-6)
    return (wide * scale * gain.astype(jnp.float32)).astype(jnp.bfloat16)


def turned(t, place, theta):
    half = t.shape[-1] // 2
    angle = place.astype(jnp.float32)[:, None] * theta ** (-jnp.arange(half, dtype=jnp.float32) / half)
    cos, sin = jnp.cos(angle)[:, None], jnp.sin(angle)[:, None]
    a, b = t[..., :half].astype(jnp.float32), t[..., half:].astype(jnp.float32)
    return jnp.concatenate([a * cos - b * sin, b * cos + a * sin], -1).astype(jnp.bfloat16)


def matmul(a, w):
    return jnp.dot(a, w, preferred_element_type=jnp.float32).astype(jnp.bfloat16)


def einsum(form, a, b):
    return jnp.einsum(form, a.astype(jnp.float32), b.astype(jnp.float32))


def attention(q, k, v):
    scores = einsum("tgsd,ugd->gstu", q, k) * q.shape[-1] ** -0.5
    token = jnp.arange(q.shape[0])
    scores = jnp.where(token[:, None] >= token, scores, -jnp.inf)
    weights = jax.nn.softmax(scores, -1).astype(jnp.bfloat16)
    return einsum("gstu,ugd->tgsd", weights, v).astype(jnp.bfloat16)


def reference(x, gain, wq, wk, wv, wo):
    a, place = normed(x, gain), jnp.arange(ROWS)
    q = turned(matmul(a, wq).reshape(ROWS, HEADS, HEAD), place, THETA).reshape(ROWS, KV_HEADS, -1, HEAD)
    k = turned(matmul(a, wk).reshape(ROWS, KV_HEADS, HEAD), place, THETA)
    v = matmul(a, wv).reshape(ROWS, KV_HEADS, HEAD)
    seen = attention(q, k, v).reshape(ROWS, HEADS * HEAD)
    return (x.astype(jnp.float32) + jnp.dot(seen, wo, preferred_element_type=jnp.float32)).astype(jnp.bfloat16)
```

```python
import functools

import jax
import jax.numpy as jnp
from jax import lax
from jax.experimental import pallas as pl
from jax.experimental.pallas import tpu as pltpu
from jax.sharding import PartitionSpec as P

HEAD = 128
THETA = 10000
LOG2E = 1.4426950408889634
OWN = 128
ROWS = 256
GROUP = 4
WIDE = GROUP * HEAD
COLS = GROUP * ROWS
STRIP = 512
MESH = pl.DeviceIdType.MESH


def _dot(a, b, ca=1, cb=0):
    return lax.dot_general(a, b, (((ca,), (cb,)), ((), ())), preferred_element_type=jnp.float32)


def _kernel(x_ref, gain_ref, cos_ref, sin_ref, wq_ref, wk_ref, wv_ref, wo_ref, y_ref,
            xs, a_s, w_s, kvsend, kv, qsend, qall, top_s, acc_s, osend, oall, ysum, yrecv,
            x_sem, w_sem, wo_sem, xs_send, xs_recv, kvp_send, kv_recv, kvz_send, fwd_send,
            q_send, q_recv, o_send, o_recv, y_send, y_recv):
    dim = x_ref.shape[1]
    tiles = dim // WIDE
    me = lax.axis_index("sp")
    c = lax.rem(me, 2)
    z = lax.rem(lax.div(me, 2), 4)
    p = lax.div(me, 8)
    px, py = lax.div(p, 2), lax.rem(p, 2)

    def flip(k):
        kx, ky = (k // 2, k % 2) if isinstance(k, int) else (lax.div(k, 2), lax.rem(k, 2))
        return 2 * (px + kx - 2 * px * kx) + (py + ky - 2 * py * ky)

    def at(p_, z_, c_):
        return {"sp": (p_ * 4 + z_) * 2 + c_}

    def send(src, dst, send_sem, recv_sem, device):
        return pltpu.make_async_remote_copy(src_ref=src, dst_ref=dst, send_sem=send_sem, recv_sem=recv_sem,
                                            device_id=device, device_id_type=MESH)

    x_copy = pltpu.make_async_copy(x_ref, xs.at[c], x_sem)
    wk_copy = pltpu.make_async_copy(wk_ref.at[:, pl.ds(pl.multiple_of(c * WIDE, WIDE), WIDE)], w_s.at[0], w_sem.at[0])
    wv_copy = pltpu.make_async_copy(wv_ref.at[:, pl.ds(pl.multiple_of(c * WIDE, WIDE), WIDE)], w_s.at[1], w_sem.at[1])

    def wq_copy(i):
        first = pl.multiple_of((c * 4 + flip(3 - i)) * WIDE, WIDE)
        return pltpu.make_async_copy(wq_ref.at[:, pl.ds(first, WIDE)], w_s.at[2 + i], w_sem.at[2 + i])

    def wo_start(k):
        first = pl.multiple_of((c * 4 + flip(k)) * WIDE, WIDE)
        for j in range(tiles):
            pltpu.make_async_copy(wo_ref.at[pl.ds(first, WIDE), pl.ds(j * WIDE, WIDE)],
                                  w_s.at[k, pl.ds(j * WIDE, WIDE), :], wo_sem.at[k]).start()

    def wo_wait(k):
        pltpu.make_async_copy(w_s.at[k], w_s.at[k], wo_sem.at[k]).wait()

    x_copy.start()
    wk_copy.start()
    wv_copy.start()

    barrier = pltpu.get_barrier_semaphore()
    pl.semaphore_signal(barrier, inc=1, device_id=at(p, z, 1 - c), device_id_type=MESH)
    for k in (1, 2, 3):
        pl.semaphore_signal(barrier, inc=1, device_id=at(flip(k), z, c), device_id_type=MESH)
    for step in (-2, -1, 1, 2):
        @pl.when((z + step >= 0) & (z + step <= 3))
        def _():
            pl.semaphore_signal(barrier, inc=1, device_id=at(p, z + step, c), device_id_type=MESH)
    pl.semaphore_wait(barrier, 6 + lax.div(z * (3 - z), 2))

    x_send = send(x_ref, xs.at[c], xs_send, xs_recv, at(p, z, 1 - c))
    x_send.start()
    wq_copy(0).start()

    def norm_rows(half):
        def rows(i, _):
            wide = xs[half, pl.ds(pl.multiple_of(i * 16, 16), 16), :].astype(jnp.float32)
            scale = lax.rsqrt(jnp.mean(wide * wide, -1, keepdims=True) + 1e-6)
            a_s[pl.ds(pl.multiple_of(half * OWN + i * 16, 16), 16), :] = (wide * scale * gain_ref[...].astype(jnp.float32)).astype(jnp.bfloat16)
        lax.fori_loop(0, OWN // 16, rows, None)

    x_copy.wait()
    norm_rows(c)
    pltpu.make_async_remote_copy(src_ref=x_ref, dst_ref=xs.at[1 - c], send_sem=xs_send, recv_sem=xs_recv,
                                 device_id=at(p, z, 1 - c), device_id_type=MESH).wait_recv()
    norm_rows(1 - c)

    def turned(t):
        t = t.astype(jnp.bfloat16).astype(jnp.float32)
        return (t * cos_ref[...] + pltpu.roll(t, HEAD // 2, 1) * sin_ref[...]).astype(jnp.bfloat16)

    wk_copy.wait()
    wv_copy.wait()
    wq_copy(1).start()
    wq_copy(2).start()
    wq_copy(3).start()

    def make_kv(j, _):
        columns = pl.ds(pl.multiple_of(j * 2 * HEAD, 2 * HEAD), 2 * HEAD)
        k = _dot(a_s[...], w_s[0, :, columns])
        v = _dot(a_s[...], w_s[1, :, columns]).astype(jnp.bfloat16)
        for n in range(2):
            kvsend[2 * j + n, 0:ROWS, :] = turned(k[:, n * HEAD : (n + 1) * HEAD])
            flat = v[:, n * HEAD : (n + 1) * HEAD].T
            kvsend[2 * j + n, ROWS : ROWS + HEAD, :] = flat[:, :HEAD]
            kvsend[2 * j + n, ROWS + HEAD : 2 * ROWS, :] = flat[:, HEAD:]

    lax.fori_loop(0, 2, make_kv, None)
    kv[4 * p + z] = kvsend[p]

    def kvp(k):
        to = flip(k)
        return send(kvsend.at[to], kv.at[4 * p + z], kvp_send.at[k - 1], kv_recv.at[4 * p + z], at(to, z, c))

    def kv_arrival(block):
        return send(kv.at[block], kv.at[block], fwd_send.at[0], kv_recv.at[block], at(p, z, c))

    def along(k, act):
        from_ = flip(k)
        block = 4 * from_ + z
        for n, step in enumerate((1, 2, -1, -2)):
            ok = (z + step <= 3) if step > 0 else ((z + step >= 0) & (from_ < 3))

            @pl.when(ok)
            def _():
                act(send(kv.at[block], kv.at[block], kvz_send.at[4 * k + n], kv_recv.at[block], at(p, z + step, c)))

    for k in (3, 2, 1):
        kvp(k).start()

    def make_q(i, _):
        wq_copy(i).wait()

        def part(j, _):
            columns = pl.ds(pl.multiple_of(j * 2 * HEAD, 2 * HEAD), 2 * HEAD)
            q = _dot(a_s[...], w_s[2 + i, :, columns])
            for n in range(2):
                qsend[i, 2 * j + n] = turned(q[:, n * HEAD : (n + 1) * HEAD])

        @pl.when(i == 0)
        def _():
            along(0, lambda copy: copy.start())

        lax.fori_loop(0, 2, part, None)

        @pl.when(i < 3)
        def _():
            to = flip(3 - i)
            send(qsend.at[i], qall.at[p], q_send.at[i], q_recv.at[p], at(to, z, c)).start()
            kv_arrival(4 * flip(i + 1) + z).wait_recv()
            along(i + 1, lambda copy: copy.start())

    lax.fori_loop(0, 4, make_q, None)
    qall[p] = qsend[3]
    for k in range(4):
        wo_start(k)

    for b in range(4):
        top_s[b] = jnp.full((1, COLS), -jnp.inf, jnp.float32)
        acc_s[b] = jnp.zeros((HEAD + 8, COLS), jnp.float32)

    def zero(j, _):
        ysum[j] = jnp.zeros((2, OWN, WIDE), jnp.float32)

    lax.fori_loop(0, tiles, zero, None)
    e = HEAD**-0.5 * LOG2E
    pieces = range(0, COLS, STRIP)

    def block(b, j, masked):
        keys = kv[j, 0:ROWS, :]
        q = qall[b].reshape(COLS, HEAD)
        scores = [_dot(keys, q[n : n + STRIP, :], 1, 1) for n in pieces]
        flat = jnp.concatenate([kv[j, ROWS : ROWS + HEAD, :], kv[j, ROWS + HEAD : 2 * ROWS, :]], axis=1)
        values = jnp.concatenate([flat, jnp.ones((8, ROWS), jnp.bfloat16)], axis=0)
        if masked:
            ok = (lax.rem(lax.broadcasted_iota(jnp.int32, (ROWS, STRIP), 1), ROWS)
                  >= lax.broadcasted_iota(jnp.int32, (ROWS, STRIP), 0))
        weights, keeps = [], []
        for n, s in zip(pieces, scores):
            if masked:
                s = jnp.where(ok, s, -jnp.inf)
            old = top_s[b, :, n : n + STRIP]
            top = jnp.maximum(old, s.max(axis=0, keepdims=True))
            top_s[b, :, n : n + STRIP] = top
            weights.append(jnp.exp2((s - top) * e).astype(jnp.bfloat16))
            keeps.append(jnp.exp2((old - top) * e))
        for n, w, keep in zip(pieces, weights, keeps):
            acc_s[b, :, n : n + STRIP] = acc_s[b, :, n : n + STRIP] * keep + _dot(values, w)

    def fwd(k, zz, step):
        j = 4 * flip(k) + zz
        return send(kv.at[j], kv.at[j], fwd_send.at[k], kv_recv.at[j], at(p, z + step, c))

    for k in (1, 2, 3):
        q_from = flip(k)
        send(qall.at[q_from], qall.at[q_from], q_send.at[0], q_recv.at[q_from], at(p, z, c)).wait_recv()

    def attend(t, _):
        g, k = lax.div(t, 4), lax.rem(t, 4)
        zz = z + lax.div(g + 1, 2) * (1 - 2 * lax.rem(g, 2))
        pp = flip(k)
        j = 4 * pp + zz

        @pl.when((zz >= 0) & (zz <= 3) & ((zz <= z) | (pp < 3)))
        def _():
            @pl.when(g > 0)
            def _():
                kv_arrival(j).wait_recv()

            @pl.when((z == 2) & (zz == 0))
            def _():
                fwd(k, 0, 1).start()

            @pl.when((z == 1) & (zz == 3))
            def _():
                fwd(k, 3, -1).start()

            @pl.when(g == 0)
            def _():
                block(pp, j, True)

            lax.fori_loop(pp + jnp.where(zz >= z, 1, 0), 4, lambda b, _: block(b, j, False), None)

    lax.fori_loop(0, 28, attend, None)

    def finish(b, out, i):
        total = acc_s[b, HEAD : HEAD + 1, :]
        out[i] = (acc_s[b, :HEAD, :] * (1 / total)).T.reshape(GROUP, ROWS, HEAD).astype(jnp.bfloat16)

    def o_copy(k):
        to = flip(k)
        return send(osend.at[k - 1], oall.at[p], o_send.at[k - 1], o_recv.at[p], at(to, z, c))

    def finish_all(i, _):
        k = 3 - i
        finish(flip(k), osend, k - 1)
        o_copy(k).start()

    lax.fori_loop(0, 3, finish_all, None)
    finish(p, oall, p)

    def heads(g):
        return jnp.concatenate([oall[g, n] for n in range(GROUP)], axis=1)

    def partial(k, _):
        g = flip(k)

        @pl.when(k > 0)
        def _():
            send(oall.at[g], oall.at[g], o_send.at[0], o_recv.at[g], at(p, z, c)).wait_recv()

        wo_wait(k)
        o = heads(g)

        def tile(j, _):
            got = _dot(o, w_s[k, pl.ds(pl.multiple_of(j * WIDE, WIDE), WIDE), :])
            ysum[j] = ysum[j] + got.reshape(2, OWN, WIDE)

        lax.fori_loop(0, tiles, tile, None)

    lax.fori_loop(0, 3, partial, None)

    def y_copy(j):
        return send(ysum.at[j, 1 - c], yrecv.at[j], y_send.at[j], y_recv.at[j], at(p, z, 1 - c))

    g = flip(3)
    send(oall.at[g], oall.at[g], o_send.at[0], o_recv.at[g], at(p, z, c)).wait_recv()
    wo_wait(3)
    o = heads(g)

    def last(j, _):
        got = _dot(o, w_s[3, pl.ds(pl.multiple_of(j * WIDE, WIDE), WIDE), :])
        ysum[j] = ysum[j] + got.reshape(2, OWN, WIDE)

        @pl.when(j > 0)
        def _():
            y_copy(j - 1).start()

    lax.fori_loop(0, tiles, last, None)
    y_copy(tiles - 1).start()

    def out(j, _):
        columns = pl.ds(pl.multiple_of(j * WIDE, WIDE), WIDE)
        y_copy(j).wait_recv()
        y_ref[:, columns] = (xs[c, :, columns].astype(jnp.float32) + (ysum[j, c] + yrecv[j])).astype(jnp.bfloat16)

    lax.fori_loop(0, tiles, out, None)

    x_send.wait_send()
    for k in (1, 2, 3):
        kvp(k).wait_send()
        o_copy(k).wait_send()
        send(qsend.at[3 - k], qall.at[p], q_send.at[3 - k], q_recv.at[p], at(flip(k), z, c)).wait_send()

    def sent(k, _):
        along(k, lambda copy: copy.wait_send())

        @pl.when(z == 2)
        def _():
            fwd(k, 0, 1).wait_send()

        @pl.when((z == 1) & (flip(k) < 3))
        def _():
            fwd(k, 3, -1).wait_send()

    lax.fori_loop(0, 4, sent, None)
    lax.fori_loop(0, tiles, lambda j, _: y_copy(j).wait_send(), None)


def layer(x, gain, cos, sin, wq, wk, wv, wo):
    dim = x.shape[1]
    tiles = dim // WIDE
    bf16, f32 = jnp.bfloat16, jnp.float32
    dma = pltpu.SemaphoreType.DMA
    vmem = pl.BlockSpec(memory_space=pltpu.VMEM)
    hbm = pl.BlockSpec(memory_space=pl.ANY)
    return pl.pallas_call(
        _kernel,
        out_shape=jax.ShapeDtypeStruct(x.shape, bf16),
        in_specs=[hbm, vmem, vmem, vmem, hbm, hbm, hbm, hbm],
        out_specs=vmem,
        scratch_shapes=[
            pltpu.VMEM((2, OWN, dim), bf16),
            pltpu.VMEM((ROWS, dim), bf16),
            pltpu.VMEM((6, dim, WIDE), bf16),
            pltpu.VMEM((4, 2 * ROWS, HEAD), bf16),
            pltpu.VMEM((16, 2 * ROWS, HEAD), bf16),
            pltpu.VMEM((4, GROUP, ROWS, HEAD), bf16),
            pltpu.VMEM((4, GROUP, ROWS, HEAD), bf16),
            pltpu.VMEM((4, 1, COLS), f32),
            pltpu.VMEM((4, HEAD + 8, COLS), f32),
            pltpu.VMEM((3, GROUP, ROWS, HEAD), bf16),
            pltpu.VMEM((4, GROUP, ROWS, HEAD), bf16),
            pltpu.VMEM((tiles, 2, OWN, WIDE), f32),
            pltpu.VMEM((tiles, OWN, WIDE), f32),
            dma, dma((6,)), dma((4,)), dma, dma, dma((3,)), dma((16,)), dma((16,)), dma((4,)),
            dma((3,)), dma((4,)), dma((3,)), dma((4,)), dma((tiles,)), dma((tiles,)),
        ],
        compiler_params=pltpu.CompilerParams(collective_id=0, has_side_effects=True, vmem_limit_bytes=63 * 2**20),
        cost_estimate=pl.CostEstimate(flops=20 * 10**9, bytes_accessed=60 * 10**6, transcendentals=10**7),
    )(x, gain, cos, sin, wq, wk, wv, wo)


def solution(mesh):
    def step(x, gain, wq, wk, wv, wo):
        own = x.shape[0]
        first = lax.div(lax.axis_index("sp"), 2) * (2 * own)
        half = HEAD // 2
        place = (first + jnp.arange(2 * own)).astype(jnp.float32)
        angle = place[:, None] * THETA ** (-jnp.arange(half, dtype=jnp.float32) / half)
        cos, sin = jnp.cos(angle), jnp.sin(angle)
        return layer(x, gain[None], jnp.concatenate([cos, cos], 1), jnp.concatenate([-sin, sin], 1), wq, wk, wv, wo)

    tokens, whole = P(("dp", "sp"), None), P(None, None)
    return jax.shard_map(
        step,
        mesh=mesh,
        in_specs=(tokens, P(None), whole, whole, whole, whole),
        out_specs=tokens,
        check_vma=False,
    )
```

```python
import numpy as np

import jax
import jax.numpy as jnp
from jax import lax
from jax.experimental import pallas as pl
from jax.experimental.pallas import tpu as pltpu
from jax.sharding import PartitionSpec as P

HEAD = 128
THETA = 10000
LOG2E = 1.4426950408889634
OWN = 128
ROWS = 256
BLOCKS = 16
GROUP = 4
WIDE = GROUP * HEAD
COLS = GROUP * ROWS
STRIP = 512
PIECES = 4
MESH = pl.DeviceIdType.MESH


def _dot(a, b, ca=1, cb=0):
    return lax.dot_general(a, b, (((ca,), (cb,)), ((), ())), preferred_element_type=jnp.float32)


def _kernel(x_ref, gain_ref, near_ref, far_ref, wq_ref, wk_ref, wv_ref, wo_ref, y_ref,
            xs, a_s, w_s, near, far, turn, kvsend, kv, qsend, qall, top_s, acc_s, osend, oall, ysum,
            x_sem, w_sem, wo_sem, t_sem, xs_send, xs_recv, kvp_send, kv_recv, kvz_send, fwd_send,
            q_send, q_recv, o_send, o_recv):
    tiles = x_ref.shape[1] // WIDE
    me = lax.axis_index("sp")
    c = lax.rem(me, 2)
    z = lax.rem(lax.div(me, 2), 4)
    p = lax.div(me, 8)
    px, py = lax.div(p, 2), lax.rem(p, 2)
    middle = (z == 1) | (z == 2)

    def flip(k):
        kx, ky = (k // 2, k % 2) if isinstance(k, int) else (lax.div(k, 2), lax.rem(k, 2))
        return 2 * (px + kx - 2 * px * kx) + (py + ky - 2 * py * ky)

    def at(p_, z_, c_):
        return {"sp": (p_ * 4 + z_) * 2 + c_}

    def send(src, dst, send_sem, recv_sem, device):
        return pltpu.make_async_remote_copy(src_ref=src, dst_ref=dst, send_sem=send_sem, recv_sem=recv_sem,
                                            device_id=device, device_id_type=MESH)

    x_copy = pltpu.make_async_copy(x_ref, xs.at[c], x_sem)
    near_copy = pltpu.make_async_copy(near_ref, near, t_sem.at[0])
    far_copy = pltpu.make_async_copy(far_ref, far, t_sem.at[1])
    wk_copy = pltpu.make_async_copy(wk_ref.at[:, pl.ds(pl.multiple_of(c * WIDE, WIDE), WIDE)], w_s.at[0], w_sem.at[0])
    wv_copy = pltpu.make_async_copy(wv_ref.at[:, pl.ds(pl.multiple_of(c * WIDE, WIDE), WIDE)], w_s.at[1], w_sem.at[1])

    def wq_copy(i):
        first = pl.multiple_of((c * 4 + flip((i + 1) % 4 if isinstance(i, int) else lax.rem(i + 1, 4))) * WIDE, WIDE)
        return pltpu.make_async_copy(wq_ref.at[:, pl.ds(first, WIDE)], w_s.at[2 + i], w_sem.at[2 + i])

    def wo_start(k, core, slot):
        first = pl.multiple_of((core * 4 + flip(k)) * WIDE, WIDE)
        for j in range(tiles):
            pltpu.make_async_copy(wo_ref.at[pl.ds(first, WIDE), pl.ds(j * WIDE, WIDE)],
                                  w_s.at[slot, pl.ds(j * WIDE, WIDE), :], wo_sem.at[slot]).start()

    def wo_wait(slot):
        pltpu.make_async_copy(w_s.at[slot], w_s.at[slot], wo_sem.at[slot]).wait()

    x_copy.start()
    wk_copy.start()
    wv_copy.start()
    near_copy.start()
    far_copy.start()

    barrier = pltpu.get_barrier_semaphore()
    pl.semaphore_signal(barrier, inc=1, device_id=at(p, z, 1 - c), device_id_type=MESH)
    for k in (1, 2, 3):
        for core in (0, 1):
            pl.semaphore_signal(barrier, inc=1, device_id=at(flip(k), z, core), device_id_type=MESH)
    for step in (-2, -1, 1, 2):
        @pl.when((z + step >= 0) & (z + step <= 3))
        def _():
            pl.semaphore_signal(barrier, inc=1, device_id=at(p, z + step, c), device_id_type=MESH)
    pl.semaphore_wait(barrier, 9 + lax.div(z * (3 - z), 2))

    def x_piece(i, core):
        rows = pl.ds(i * (OWN // PIECES), OWN // PIECES)
        return send(xs.at[core, rows], xs.at[core, rows], xs_send.at[i], xs_recv.at[i], at(p, z, 1 - c))

    x_copy.wait()
    for i in range(PIECES):
        x_piece(i, c).start()
    wq_copy(0).start()

    def norm_rows(half, first, count):
        def rows(i, _):
            here = first + i * 16
            wide = xs[half, pl.ds(pl.multiple_of(here, 16), 16), :].astype(jnp.float32)
            scale = lax.rsqrt(jnp.mean(wide * wide, -1, keepdims=True) + 1e-6)
            gain = gain_ref[...].astype(jnp.float32)
            a_s[pl.ds(pl.multiple_of(half * OWN + here, 16), 16), :] = (wide * scale * gain).astype(jnp.bfloat16)
        lax.fori_loop(0, count // 16, rows, None)

    norm_rows(c, 0, OWN)
    near_copy.wait()
    far_copy.wait()
    block_no = 4 * p + z
    base_cos, base_sin = far[0, pl.ds(block_no, 1), :], far[1, pl.ds(block_no, 1), :]
    turn[0] = near[0] * base_cos - near[1] * base_sin
    turn[1] = (near[1] * base_cos + near[0] * base_sin) * far[2, 0:1, :]

    def x_arrived(i, _):
        x_piece(i, 1 - c).wait_recv()
        norm_rows(1 - c, i * (OWN // PIECES), OWN // PIECES)

    lax.fori_loop(0, PIECES, x_arrived, None)

    def turned(t):
        t = t.astype(jnp.bfloat16).astype(jnp.float32)
        return (t * turn[0] + pltpu.roll(t, HEAD // 2, 1) * turn[1]).astype(jnp.bfloat16)

    wk_copy.wait()
    wv_copy.wait()
    wq_copy(1).start()
    wq_copy(2).start()
    wq_copy(3).start()

    def make_kv(j, _):
        columns = pl.ds(pl.multiple_of(j * 2 * HEAD, 2 * HEAD), 2 * HEAD)
        k = _dot(a_s[...], w_s[0, :, columns])
        v = _dot(a_s[...], w_s[1, :, columns]).astype(jnp.bfloat16)
        for n in range(2):
            kvsend[2 * j + n, 0:ROWS, :] = turned(k[:, n * HEAD : (n + 1) * HEAD])
            flat = v[:, n * HEAD : (n + 1) * HEAD].T
            kvsend[2 * j + n, ROWS : ROWS + HEAD, :] = flat[:, :HEAD]
            kvsend[2 * j + n, ROWS + HEAD : 2 * ROWS, :] = flat[:, HEAD:]

    lax.fori_loop(0, 2, make_kv, None)
    kv[block_no] = kvsend[p]

    def kvp(k):
        to = flip(k)
        return send(kvsend.at[to], kv.at[block_no], kvp_send.at[k - 1], kv_recv.at[block_no], at(to, z, c))

    def kv_arrival(block):
        return send(kv.at[block], kv.at[block], fwd_send.at[0], kv_recv.at[block], at(p, z, c))

    def along(k, act):
        from_ = flip(k)
        block = 4 * from_ + z
        for n, step in enumerate((2, 1, -2, -1)):
            ok = (z + step <= 3) if step > 0 else ((z + step >= 0) & (from_ < 3))

            @pl.when(ok)
            def _():
                act(send(kv.at[block], kv.at[block], kvz_send.at[4 * k + n], kv_recv.at[block], at(p, z + step, c)))

    for k in (1, 2, 3):
        kvp(k).start()

    def q_copy(i, to):
        return send(qsend.at[i], qall.at[p], q_send.at[i], q_recv.at[p], at(to, z, c))

    def make_q(i, _):
        wq_copy(i).wait()

        @pl.when(i == 0)
        def _():
            along(0, lambda copy: copy.start())

        def part(j, _):
            columns = pl.ds(pl.multiple_of(j * 2 * HEAD, 2 * HEAD), 2 * HEAD)
            q = _dot(a_s[...], w_s[2 + i, :, columns])
            for n in range(2):
                qsend[i, 2 * j + n] = turned(q[:, n * HEAD : (n + 1) * HEAD])

        lax.fori_loop(0, 2, part, None)

        @pl.when(i < 3)
        def _():
            q_copy(i, flip(i + 1)).start()

        @pl.when(i > 0)
        def _():
            kv_arrival(4 * flip(i) + z).wait_recv()
            along(i, lambda copy: copy.start())

    lax.fori_loop(0, 4, make_q, None)
    qall[p] = qsend[3]
    for k in range(4):
        for n in range(2):
            core = c if n == 0 else 1 - c
            wo_start(k, core, 2 * k + n)

    for b in range(4):
        top_s[b] = jnp.full((1, COLS), -jnp.inf, jnp.float32)
        acc_s[b] = jnp.zeros((HEAD + 8, COLS), jnp.float32)

    e = HEAD**-0.5 * LOG2E
    strips = range(0, COLS, STRIP)

    def block(b, j, masked):
        keys = kv[j, 0:ROWS, :]
        q = qall[b].reshape(COLS, HEAD)
        scores = [_dot(keys, q[n : n + STRIP, :], 1, 1) for n in strips]
        flat = jnp.concatenate([kv[j, ROWS : ROWS + HEAD, :], kv[j, ROWS + HEAD : 2 * ROWS, :]], axis=1)
        values = jnp.concatenate([flat, jnp.ones((8, ROWS), jnp.bfloat16)], axis=0)
        if masked:
            ok = (lax.rem(lax.broadcasted_iota(jnp.int32, (ROWS, STRIP), 1), ROWS)
                  >= lax.broadcasted_iota(jnp.int32, (ROWS, STRIP), 0))
        weights, keeps = [], []
        for n, s in zip(strips, scores):
            if masked:
                s = jnp.where(ok, s, -jnp.inf)
            old = top_s[b, :, n : n + STRIP]
            top = jnp.maximum(old, s.max(axis=0, keepdims=True))
            top_s[b, :, n : n + STRIP] = top
            weights.append(jnp.exp2((s - top) * e).astype(jnp.bfloat16))
            keeps.append(jnp.exp2((old - top) * e))
        for n, w, keep in zip(strips, weights, keeps):
            acc_s[b, :, n : n + STRIP] = acc_s[b, :, n : n + STRIP] * keep + _dot(values, w)

    def unit(t):
        g, k = lax.div(t, 4), lax.rem(t, 4)
        low = jnp.where(z < 2, z, 3 - z)
        zz = jnp.where((low == 1) & (g < 2), 1 - g, g)
        zz = jnp.where(z < 2, zz, 3 - zz)
        pp = flip(k)
        return pp, zz, 4 * pp + zz

    def fwd(k, zz, step):
        j = 4 * flip(k) + zz
        return send(kv.at[j], kv.at[j], fwd_send.at[k], kv_recv.at[j], at(p, z + step, c))

    def arrive(t):
        pp, zz, j = unit(t)

        @pl.when((zz <= z) | (pp < 3))
        def _():
            kv_arrival(j).wait_recv()

            @pl.when((z == 2) & (zz == 0))
            def _():
                fwd(lax.rem(t, 4), 0, 1).start()

            @pl.when((z == 1) & (zz == 3))
            def _():
                fwd(lax.rem(t, 4), 3, -1).start()

    def visit(t, first, last, own):
        pp, zz, j = unit(t)

        def one(k, _):
            b = flip(k)

            @pl.when((pp < b) | ((pp == b) & (zz < z)))
            def _():
                block(b, j, False)

            if own:
                @pl.when((pp == b) & (zz == z))
                def _():
                    block(b, j, True)

        lax.fori_loop(first, last, one, None)

    def q_arrive(k):
        q_from = flip(k)
        send(qall.at[q_from], qall.at[q_from], q_send.at[0], q_recv.at[q_from], at(p, z, c)).wait_recv()

    def own_first(t, _):
        @pl.when(t > 3)
        def _():
            arrive(t)

        visit(t, 0, 1, True)

    lax.fori_loop(0, 8, own_first, None)
    q_arrive(1)
    q_arrive(2)
    lax.fori_loop(0, 8, lambda t, _: visit(t, 1, 3, True), None)
    q_arrive(3)
    lax.fori_loop(0, 8, lambda t, _: visit(t, 3, 4, True), None)

    def rest(t, _):
        @pl.when((t < 12) | (z == 0) | (z == 3))
        def _():
            arrive(t)

        @pl.when((t < 12) & middle)
        def _():
            arrive(t + 4)

        visit(t, 0, 4, False)

    lax.fori_loop(8, 16, rest, None)

    def finish(b):
        total = acc_s[b, HEAD : HEAD + 1, :]
        return (acc_s[b, :HEAD, :] * (1 / total)).T.reshape(GROUP, 2, OWN, HEAD).astype(jnp.bfloat16)

    def o_copy(k, core):
        return send(osend.at[k, core], oall.at[p, c], o_send.at[k, core], o_recv.at[p, c], at(flip(k), z, core))

    def o_arrive(k, core):
        g = flip(k)
        send(oall.at[g, core], oall.at[g, core], o_send.at[0, 0], o_recv.at[g, core], at(p, z, c)).wait_recv()

    def finish_all(i, _):
        k = lax.rem(i + 1, 4)
        got = finish(flip(k))
        for core in range(2):
            osend[k, core] = got[:, core]

        @pl.when(k > 0)
        def _():
            for core in range(2):
                o_copy(k, core).start()

    lax.fori_loop(0, 4, finish_all, None)
    o_copy(0, 1 - c).start()
    oall[p, c] = osend[0, c]

    def heads(g, core):
        return jnp.concatenate([oall[g, core, n] for n in range(GROUP)], axis=1)

    def project(k, j, mine, other):
        rows = pl.ds(pl.multiple_of(j * WIDE, WIDE), WIDE)
        return _dot(mine, w_s[2 * k, rows, :]) + _dot(other, w_s[2 * k + 1, rows, :])

    def operands(k):
        @pl.when(k > 0)
        def _():
            o_arrive(k, c)

        o_arrive(k, 1 - c)
        wo_wait(2 * k)
        wo_wait(2 * k + 1)
        g = flip(k)
        return heads(g, c), heads(g, 1 - c)

    mine, other = operands(jnp.int32(0))

    def first_tile(j, _):
        columns = pl.ds(pl.multiple_of(j * WIDE, WIDE), WIDE)
        ysum[:, columns] = xs[c, :, columns].astype(jnp.float32) + project(0, j, mine, other)

    lax.fori_loop(0, tiles, first_tile, None)

    def middle_chips(k, _):
        mine, other = operands(k)

        def tile(j, _):
            columns = pl.ds(pl.multiple_of(j * WIDE, WIDE), WIDE)
            ysum[:, columns] = ysum[:, columns] + project(k, j, mine, other)

        lax.fori_loop(0, tiles, tile, None)

    lax.fori_loop(1, 3, middle_chips, None)
    mine3, other3 = operands(jnp.int32(3))

    def last_tile(j, _):
        columns = pl.ds(pl.multiple_of(j * WIDE, WIDE), WIDE)
        y_ref[:, columns] = (ysum[:, columns] + project(3, j, mine3, other3)).astype(jnp.bfloat16)

    lax.fori_loop(0, tiles, last_tile, None)

    for i in range(PIECES):
        x_piece(i, c).wait_send()
    for k in (1, 2, 3):
        kvp(k).wait_send()
        q_copy(k - 1, flip(k)).wait_send()
        for core in range(2):
            o_copy(k, core).wait_send()
    o_copy(0, 1 - c).wait_send()

    def sent(k, _):
        along(k, lambda copy: copy.wait_send())

        @pl.when(z == 2)
        def _():
            fwd(k, 0, 1).wait_send()

        @pl.when((z == 1) & (flip(k) < 3))
        def _():
            fwd(k, 3, -1).wait_send()

    lax.fori_loop(0, 4, sent, None)


def tables():
    half = HEAD // 2
    speed = np.tile(float(THETA) ** (-np.arange(half) / half), 2)
    near, far = np.arange(ROWS)[:, None] * speed, ROWS * np.arange(BLOCKS)[:, None] * speed
    sign = np.broadcast_to(np.where(np.arange(HEAD) < half, -1.0, 1.0), far.shape)
    return np.stack([np.cos(near), np.sin(near)]).astype(np.float32), np.stack([np.cos(far), np.sin(far), sign]).astype(np.float32)


def layer(x, gain, wq, wk, wv, wo):
    dim = x.shape[1]
    bf16, f32 = jnp.bfloat16, jnp.float32
    dma = pltpu.SemaphoreType.DMA
    vmem = pl.BlockSpec(memory_space=pltpu.VMEM)
    hbm = pl.BlockSpec(memory_space=pl.ANY)
    near, far = tables()
    return pl.pallas_call(
        _kernel,
        out_shape=jax.ShapeDtypeStruct(x.shape, bf16),
        in_specs=[hbm, vmem, hbm, hbm, hbm, hbm, hbm, hbm],
        out_specs=vmem,
        scratch_shapes=[
            pltpu.VMEM((2, OWN, dim), bf16),
            pltpu.VMEM((ROWS, dim), bf16),
            pltpu.VMEM((8, dim, WIDE), bf16),
            pltpu.VMEM(near.shape, f32),
            pltpu.VMEM(far.shape, f32),
            pltpu.VMEM((2, ROWS, HEAD), f32),
            pltpu.VMEM((4, 2 * ROWS, HEAD), bf16),
            pltpu.VMEM((BLOCKS, 2 * ROWS, HEAD), bf16),
            pltpu.VMEM((4, GROUP, ROWS, HEAD), bf16),
            pltpu.VMEM((4, GROUP, ROWS, HEAD), bf16),
            pltpu.VMEM((4, 1, COLS), f32),
            pltpu.VMEM((4, HEAD + 8, COLS), f32),
            pltpu.VMEM((4, 2, GROUP, OWN, HEAD), bf16),
            pltpu.VMEM((4, 2, GROUP, OWN, HEAD), bf16),
            pltpu.VMEM((OWN, dim), f32),
            dma, dma((6,)), dma((8,)), dma((2,)), dma((PIECES,)), dma((PIECES,)), dma((3,)), dma((BLOCKS,)), dma((16,)), dma((4,)),
            dma((3,)), dma((4,)), dma((4, 2)), dma((4, 2)),
        ],
        compiler_params=pltpu.CompilerParams(collective_id=0, has_side_effects=True, vmem_limit_bytes=63 * 2**20),
        cost_estimate=pl.CostEstimate(flops=20 * 10**9, bytes_accessed=80 * 10**6, transcendentals=10**7),
    )(x, gain, jnp.asarray(near), jnp.asarray(far), wq, wk, wv, wo)


def solution(mesh):
    def step(x, gain, wq, wk, wv, wo):
        return layer(x, gain[None], wq, wk, wv, wo)

    tokens, whole = P(("dp", "sp"), None), P(None, None)
    return jax.shard_map(
        step,
        mesh=mesh,
        in_specs=(tokens, P(None), whole, whole, whole, whole),
        out_specs=tokens,
        check_vma=False,
    )
```

```python
import numpy as np

import jax
import jax.numpy as jnp
from jax import lax
from jax.experimental import pallas as pl
from jax.experimental.pallas import tpu as pltpu
from jax.sharding import PartitionSpec as P

HEAD = 128
THETA = 10000
LOG2E = 1.4426950408889634
OWN = 128
ROWS = 256
BLOCKS = 16
GROUP = 4
WIDE = GROUP * HEAD
COLS = GROUP * ROWS
STRIP = 512
PIECES = 4
MESH = pl.DeviceIdType.MESH


def _dot(a, b, ca=1, cb=0):
    return lax.dot_general(a, b, (((ca,), (cb,)), ((), ())), preferred_element_type=jnp.float32)


def _kernel(x_ref, gain_ref, near_ref, far_ref, wq_ref, wk_ref, wv_ref, wo_ref, y_ref,
            xs, a_s, w_s, near, far, turn, kvsend, kv, qsend, qall, top_s, acc_s, osend, oall, ysum,
            x_sem, w_sem, wo_sem, t_sem, xs_send, xs_recv, kvp_send, kv_recv, kvz_send, fwd_send,
            q_send, q_recv, o_send, o_recv):
    tiles = x_ref.shape[1] // WIDE
    me = lax.axis_index("sp")
    c = lax.rem(me, 2)
    z = lax.rem(lax.div(me, 2), 4)
    p = lax.div(me, 8)
    px, py = lax.div(p, 2), lax.rem(p, 2)
    middle = (z == 1) | (z == 2)

    def flip(k):
        kx, ky = (k // 2, k % 2) if isinstance(k, int) else (lax.div(k, 2), lax.rem(k, 2))
        return 2 * (px + kx - 2 * px * kx) + (py + ky - 2 * py * ky)

    def at(p_, z_, c_):
        return {"sp": (p_ * 4 + z_) * 2 + c_}

    def send(src, dst, send_sem, recv_sem, device):
        return pltpu.make_async_remote_copy(src_ref=src, dst_ref=dst, send_sem=send_sem, recv_sem=recv_sem,
                                            device_id=device, device_id_type=MESH)

    x_copy = pltpu.make_async_copy(x_ref, xs.at[c], x_sem)
    near_copy = pltpu.make_async_copy(near_ref, near, t_sem.at[0])
    far_copy = pltpu.make_async_copy(far_ref, far, t_sem.at[1])
    wk_copy = pltpu.make_async_copy(wk_ref.at[:, pl.ds(pl.multiple_of(c * WIDE, WIDE), WIDE)], w_s.at[0], w_sem.at[0])
    wv_copy = pltpu.make_async_copy(wv_ref.at[:, pl.ds(pl.multiple_of(c * WIDE, WIDE), WIDE)], w_s.at[1], w_sem.at[1])

    def wq_copy(i):
        first = pl.multiple_of((c * 4 + flip((i + 1) % 4 if isinstance(i, int) else lax.rem(i + 1, 4))) * WIDE, WIDE)
        return pltpu.make_async_copy(wq_ref.at[:, pl.ds(first, WIDE)], w_s.at[2 + i], w_sem.at[2 + i])

    def wo_start(k, core, slot):
        first = pl.multiple_of((core * 4 + flip(k)) * WIDE, WIDE)
        for j in range(tiles):
            pltpu.make_async_copy(wo_ref.at[pl.ds(first, WIDE), pl.ds(j * WIDE, WIDE)],
                                  w_s.at[slot, pl.ds(j * WIDE, WIDE), :], wo_sem.at[slot]).start()

    def wo_wait(slot):
        pltpu.make_async_copy(w_s.at[slot], w_s.at[slot], wo_sem.at[slot]).wait()

    x_copy.start()
    wk_copy.start()
    wv_copy.start()
    near_copy.start()
    far_copy.start()

    barrier = pltpu.get_barrier_semaphore()
    pl.semaphore_signal(barrier, inc=1, device_id=at(p, z, 1 - c), device_id_type=MESH)
    for k in (1, 2, 3):
        for core in (0, 1):
            pl.semaphore_signal(barrier, inc=1, device_id=at(flip(k), z, core), device_id_type=MESH)
    for step in (-1, 1):
        @pl.when((z + step >= 0) & (z + step <= 3))
        def _():
            pl.semaphore_signal(barrier, inc=1, device_id=at(p, z + step, c), device_id_type=MESH)
    pl.semaphore_wait(barrier, 8 + lax.div(z * (3 - z), 2))

    def x_piece(i, core):
        rows = pl.ds(i * (OWN // PIECES), OWN // PIECES)
        return send(xs.at[core, rows], xs.at[core, rows], xs_send.at[i], xs_recv.at[i], at(p, z, 1 - c))

    x_copy.wait()
    for i in range(PIECES):
        x_piece(i, c).start()
    wq_copy(0).start()

    def norm_rows(half, first, count):
        def rows(i, _):
            here = first + i * 16
            wide = xs[half, pl.ds(pl.multiple_of(here, 16), 16), :].astype(jnp.float32)
            scale = lax.rsqrt(jnp.mean(wide * wide, -1, keepdims=True) + 1e-6)
            gain = gain_ref[...].astype(jnp.float32)[None]
            a_s[pl.ds(pl.multiple_of(half * OWN + here, 16), 16), :] = (wide * scale * gain).astype(jnp.bfloat16)
        lax.fori_loop(0, count // 16, rows, None)

    norm_rows(c, 0, OWN)
    near_copy.wait()
    far_copy.wait()
    block_no = 4 * p + z
    base_cos, base_sin = far[0, pl.ds(block_no, 1), :], far[1, pl.ds(block_no, 1), :]
    turn[0] = near[0] * base_cos - near[1] * base_sin
    turn[1] = (near[1] * base_cos + near[0] * base_sin) * far[2, 0:1, :]

    def x_arrived(i, _):
        x_piece(i, 1 - c).wait_recv()
        norm_rows(1 - c, i * (OWN // PIECES), OWN // PIECES)

    lax.fori_loop(0, PIECES, x_arrived, None)

    def turned(t):
        t = t.astype(jnp.bfloat16).astype(jnp.float32)
        return (t * turn[0] + pltpu.roll(t, HEAD // 2, 1) * turn[1]).astype(jnp.bfloat16)

    wk_copy.wait()
    wv_copy.wait()
    wq_copy(1).start()
    wq_copy(2).start()
    wq_copy(3).start()

    def make_kv(j, _):
        columns = pl.ds(pl.multiple_of(j * 2 * HEAD, 2 * HEAD), 2 * HEAD)
        k = _dot(a_s[...], w_s[0, :, columns])
        v = _dot(a_s[...], w_s[1, :, columns]).astype(jnp.bfloat16)
        for n in range(2):
            kvsend[2 * j + n, 0:ROWS, :] = turned(k[:, n * HEAD : (n + 1) * HEAD])
            flat = v[:, n * HEAD : (n + 1) * HEAD].T
            kvsend[2 * j + n, ROWS : ROWS + HEAD, :] = flat[:, :HEAD]
            kvsend[2 * j + n, ROWS + HEAD : 2 * ROWS, :] = flat[:, HEAD:]

    lax.fori_loop(0, 2, make_kv, None)
    kv[block_no] = kvsend[p]

    def kvp(k):
        to = flip(k)
        return send(kvsend.at[to], kv.at[block_no], kvp_send.at[k - 1], kv_recv.at[block_no], at(to, z, c))

    def kv_arrival(block):
        return send(kv.at[block], kv.at[block], fwd_send.at[0], kv_recv.at[block], at(p, z, c))

    def along(k, act):
        from_ = flip(k)
        block = 4 * from_ + z
        for n, step in enumerate((1, -1)):
            ok = (z + step <= 3) if step > 0 else ((z + step >= 0) & (from_ < 3))

            @pl.when(ok)
            def _():
                act(send(kv.at[block], kv.at[block], kvz_send.at[2 * k + n], kv_recv.at[block], at(p, z + step, c)))

    for k in (1, 2, 3):
        kvp(k).start()

    def q_copy(i, to):
        return send(qsend.at[i], qall.at[p], q_send.at[i], q_recv.at[p], at(to, z, c))

    def make_q(i, _):
        wq_copy(i).wait()

        @pl.when(i == 0)
        def _():
            along(0, lambda copy: copy.start())

        def part(j, _):
            columns = pl.ds(pl.multiple_of(j * 2 * HEAD, 2 * HEAD), 2 * HEAD)
            q = _dot(a_s[...], w_s[2 + i, :, columns])
            for n in range(2):
                qsend[i, 2 * j + n] = turned(q[:, n * HEAD : (n + 1) * HEAD])

        lax.fori_loop(0, 2, part, None)

        @pl.when(i < 3)
        def _():
            q_copy(i, flip(i + 1)).start()

        @pl.when(i > 0)
        def _():
            kv_arrival(4 * flip(i) + z).wait_recv()
            along(i, lambda copy: copy.start())

    lax.fori_loop(0, 4, make_q, None)
    qall[p] = qsend[3]
    for k in range(4):
        for n in range(2):
            core = c if n == 0 else 1 - c
            wo_start(k, core, 2 * k + n)

    for b in range(4):
        top_s[b] = jnp.full((1, COLS), -jnp.inf, jnp.float32)
        acc_s[b] = jnp.zeros((HEAD + 8, COLS), jnp.float32)

    e = HEAD**-0.5 * LOG2E
    strips = range(0, COLS, STRIP)

    def block(b, j, masked):
        keys = kv[j, 0:ROWS, :]
        q = qall[b].reshape(COLS, HEAD)
        scores = [_dot(keys, q[n : n + STRIP, :], 1, 1) for n in strips]
        flat = jnp.concatenate([kv[j, ROWS : ROWS + HEAD, :], kv[j, ROWS + HEAD : 2 * ROWS, :]], axis=1)
        values = jnp.concatenate([flat, jnp.ones((8, ROWS), jnp.bfloat16)], axis=0)
        if masked:
            ok = (lax.rem(lax.broadcasted_iota(jnp.int32, (ROWS, STRIP), 1), ROWS)
                  >= lax.broadcasted_iota(jnp.int32, (ROWS, STRIP), 0))
        weights, keeps = [], []
        for n, s in zip(strips, scores):
            if masked:
                s = jnp.where(ok, s, -jnp.inf)
            old = top_s[b, :, n : n + STRIP]
            top = jnp.maximum(old, s.max(axis=0, keepdims=True))
            top_s[b, :, n : n + STRIP] = top
            weights.append(jnp.exp2((s - top) * e).astype(jnp.bfloat16))
            keeps.append(jnp.exp2((old - top) * e))
        for n, w, keep in zip(strips, weights, keeps):
            acc_s[b, :, n : n + STRIP] = acc_s[b, :, n : n + STRIP] * keep + _dot(values, w)

    def unit(t):
        g, k = lax.div(t, 4), lax.rem(t, 4)
        inner = jnp.where(z == 1, jnp.where(g < 2, 1 - g, g), jnp.where(g < 2, 2 - g, 9 - 3 * g))
        zz = jnp.where(middle, inner, jnp.where(z == 0, g, 3 - g))
        pp = flip(k)
        return pp, zz, 4 * pp + zz

    def forward(t, act):
        pp, zz, j = unit(t)
        for step, ok in ((1, (zz < z) & (z < 3)), (-1, (zz > z) & (z > 0) & (pp < 3))):
            @pl.when(ok)
            def _():
                act(send(kv.at[j], kv.at[j], fwd_send.at[j], kv_recv.at[j], at(p, z + step, c)))

    def arrive(t):
        pp, zz, j = unit(t)

        @pl.when((zz <= z) | (pp < 3))
        def _():
            kv_arrival(j).wait_recv()

        forward(t, lambda copy: copy.start())

    def visit(t, first, last, own):
        pp, zz, j = unit(t)

        def one(k, _):
            b = flip(k)

            @pl.when((pp < b) | ((pp == b) & (zz < z)))
            def _():
                block(b, j, False)

            if own:
                @pl.when((pp == b) & (zz == z))
                def _():
                    block(b, j, True)

        lax.fori_loop(first, last, one, None)

    def q_arrive(k):
        q_from = flip(k)
        send(qall.at[q_from], qall.at[q_from], q_send.at[0], q_recv.at[q_from], at(p, z, c)).wait_recv()

    def own_first(t, _):
        @pl.when(t > 3)
        def _():
            arrive(t)

        visit(t, 0, 1, True)

    lax.fori_loop(0, 8, own_first, None)

    @pl.when(middle)
    def _():
        lax.fori_loop(8, 12, lambda t, _: arrive(t), None)

    q_arrive(1)
    q_arrive(2)
    lax.fori_loop(0, 8, lambda t, _: visit(t, 1, 3, True), None)
    q_arrive(3)
    lax.fori_loop(0, 8, lambda t, _: visit(t, 3, 4, True), None)

    def rest(t, _):
        @pl.when((z == 0) | (z == 3))
        def _():
            arrive(t)

        @pl.when((t < 12) & middle)
        def _():
            arrive(t + 4)

        visit(t, 0, 4, False)

    lax.fori_loop(8, 16, rest, None)

    def finish(b):
        total = acc_s[b, HEAD : HEAD + 1, :]
        return (acc_s[b, :HEAD, :] * (1 / total)).T.reshape(GROUP, 2, OWN, HEAD).astype(jnp.bfloat16)

    def o_copy(k, core):
        return send(osend.at[k, core], oall.at[p, c], o_send.at[k, core], o_recv.at[p, c], at(flip(k), z, core))

    def o_arrive(k, core):
        g = flip(k)
        send(oall.at[g, core], oall.at[g, core], o_send.at[0, 0], o_recv.at[g, core], at(p, z, c)).wait_recv()

    def finish_all(i, _):
        k = lax.rem(i + 1, 4)
        got = finish(flip(k))
        for core in range(2):
            osend[k, core] = got[:, core]

        @pl.when(k > 0)
        def _():
            for core in range(2):
                o_copy(k, core).start()

    lax.fori_loop(0, 4, finish_all, None)
    o_copy(0, 1 - c).start()
    oall[p, c] = osend[0, c]

    def heads(g, core):
        return jnp.concatenate([oall[g, core, n] for n in range(GROUP)], axis=1)

    def project(k, j, mine, other):
        rows = pl.ds(pl.multiple_of(j * WIDE, WIDE), WIDE)
        return _dot(mine, w_s[2 * k, rows, :]) + _dot(other, w_s[2 * k + 1, rows, :])

    def operands(k):
        @pl.when(k > 0)
        def _():
            o_arrive(k, c)

        o_arrive(k, 1 - c)
        wo_wait(2 * k)
        wo_wait(2 * k + 1)
        g = flip(k)
        return heads(g, c), heads(g, 1 - c)

    mine, other = operands(jnp.int32(0))

    def first_tile(j, _):
        columns = pl.ds(pl.multiple_of(j * WIDE, WIDE), WIDE)
        ysum[:, columns] = xs[c, :, columns].astype(jnp.float32) + project(0, j, mine, other)

    lax.fori_loop(0, tiles, first_tile, None)

    def middle_chips(k, _):
        mine, other = operands(k)

        def tile(j, _):
            columns = pl.ds(pl.multiple_of(j * WIDE, WIDE), WIDE)
            ysum[:, columns] = ysum[:, columns] + project(k, j, mine, other)

        lax.fori_loop(0, tiles, tile, None)

    lax.fori_loop(1, 3, middle_chips, None)
    mine3, other3 = operands(jnp.int32(3))

    def last_tile(j, _):
        columns = pl.ds(pl.multiple_of(j * WIDE, WIDE), WIDE)
        y_ref[:, columns] = (ysum[:, columns] + project(3, j, mine3, other3)).astype(jnp.bfloat16)

    lax.fori_loop(0, tiles, last_tile, None)

    for i in range(PIECES):
        x_piece(i, c).wait_send()
    for k in (1, 2, 3):
        kvp(k).wait_send()
        q_copy(k - 1, flip(k)).wait_send()
        for core in range(2):
            o_copy(k, core).wait_send()
    o_copy(0, 1 - c).wait_send()

    def sent(k, _):
        along(k, lambda copy: copy.wait_send())

    lax.fori_loop(0, 4, sent, None)
    lax.fori_loop(4, BLOCKS, lambda t, _: forward(t, lambda copy: copy.wait_send()), None)


def tables():
    half = HEAD // 2
    speed = np.tile(float(THETA) ** (-np.arange(half) / half), 2)
    near, far = np.arange(ROWS)[:, None] * speed, ROWS * np.arange(BLOCKS)[:, None] * speed
    sign = np.broadcast_to(np.where(np.arange(HEAD) < half, -1.0, 1.0), far.shape)
    return np.stack([np.cos(near), np.sin(near)]).astype(np.float32), np.stack([np.cos(far), np.sin(far), sign]).astype(np.float32)


def layer(x, gain, wq, wk, wv, wo):
    dim = x.shape[1]
    bf16, f32 = jnp.bfloat16, jnp.float32
    dma = pltpu.SemaphoreType.DMA
    vmem = pl.BlockSpec(memory_space=pltpu.VMEM)
    hbm = pl.BlockSpec(memory_space=pl.ANY)
    near, far = tables()
    return pl.pallas_call(
        _kernel,
        out_shape=pltpu.VMEM(x.shape, bf16),
        in_specs=[hbm, vmem, hbm, hbm, hbm, hbm, hbm, hbm],
        out_specs=vmem,
        scratch_shapes=[
            pltpu.VMEM((2, OWN, dim), bf16),
            pltpu.VMEM((ROWS, dim), bf16),
            pltpu.VMEM((8, dim, WIDE), bf16),
            pltpu.VMEM(near.shape, f32),
            pltpu.VMEM(far.shape, f32),
            pltpu.VMEM((2, ROWS, HEAD), f32),
            pltpu.VMEM((4, 2 * ROWS, HEAD), bf16),
            pltpu.VMEM((BLOCKS, 2 * ROWS, HEAD), bf16),
            pltpu.VMEM((4, GROUP, ROWS, HEAD), bf16),
            pltpu.VMEM((4, GROUP, ROWS, HEAD), bf16),
            pltpu.VMEM((4, 1, COLS), f32),
            pltpu.VMEM((4, HEAD + 8, COLS), f32),
            pltpu.VMEM((4, 2, GROUP, OWN, HEAD), bf16),
            pltpu.VMEM((4, 2, GROUP, OWN, HEAD), bf16),
            pltpu.VMEM((OWN, dim), f32),
            dma, dma((6,)), dma((8,)), dma((2,)), dma((PIECES,)), dma((PIECES,)), dma((3,)), dma((BLOCKS,)), dma((8,)), dma((BLOCKS,)),
            dma((3,)), dma((4,)), dma((4, 2)), dma((4, 2)),
        ],
        compiler_params=pltpu.CompilerParams(collective_id=0, has_side_effects=True, vmem_limit_bytes=61 * 2**20),
        cost_estimate=pl.CostEstimate(flops=20 * 10**9, bytes_accessed=80 * 10**6, transcendentals=10**7),
    )(x, gain, jnp.asarray(near), jnp.asarray(far), wq, wk, wv, wo)


def solution(mesh):
    def step(x, gain, wq, wk, wv, wo):
        return layer(x, gain, wq, wk, wv, wo)

    tokens, whole = P(("dp", "sp"), None), P(None, None)
    return jax.shard_map(
        step,
        mesh=mesh,
        in_specs=(tokens, P(None), whole, whole, whole, whole),
        out_specs=tokens,
        check_vma=False,
    )
```

```python
import numpy as np

import jax
import jax.numpy as jnp
from jax import lax
from jax.experimental import pallas as pl
from jax.experimental.pallas import tpu as pltpu
from jax.sharding import PartitionSpec as P

HEAD = 128
THETA = 10000
LOG2E = 1.4426950408889634
OWN = 128
ROWS = 256
BLOCKS = 16
GROUP = 4
WIDE = GROUP * HEAD
COLS = GROUP * ROWS
STRIP = 512
PIECES = 4
MESH = pl.DeviceIdType.MESH


def _dot(a, b, ca=1, cb=0):
    return lax.dot_general(a, b, (((ca,), (cb,)), ((), ())), preferred_element_type=jnp.float32)


def _kernel(x_ref, gain_ref, near_ref, far_ref, wq_ref, wk_ref, wv_ref, wo_ref, y_ref,
            xs, a_s, w_s, near, far, turn, kvsend, kv, qsend, qall, top_s, acc_s, osend, oall, ysum,
            x_sem, w_sem, wo_sem, t_sem, xs_send, xs_recv, kvp_send, kv_recv, kvz_send, fwd_send,
            q_send, q_recv, o_send, o_recv):
    tiles = x_ref.shape[1] // WIDE
    me = lax.axis_index("sp")
    c = lax.rem(me, 2)
    z = lax.rem(lax.div(me, 2), 4)
    p = lax.div(me, 8)
    px, py = lax.div(p, 2), lax.rem(p, 2)
    middle = (z == 1) | (z == 2)

    def flip(k):
        kx, ky = (k // 2, k % 2) if isinstance(k, int) else (lax.div(k, 2), lax.rem(k, 2))
        return 2 * (px + kx - 2 * px * kx) + (py + ky - 2 * py * ky)

    def at(p_, z_, c_):
        return {"sp": (p_ * 4 + z_) * 2 + c_}

    def send(src, dst, send_sem, recv_sem, device):
        return pltpu.make_async_remote_copy(src_ref=src, dst_ref=dst, send_sem=send_sem, recv_sem=recv_sem,
                                            device_id=device, device_id_type=MESH)

    x_copy = pltpu.make_async_copy(x_ref, xs.at[c], x_sem)
    near_copy = pltpu.make_async_copy(near_ref, near, t_sem.at[0])
    far_copy = pltpu.make_async_copy(far_ref, far, t_sem.at[1])
    wk_copy = pltpu.make_async_copy(wk_ref.at[:, pl.ds(pl.multiple_of(c * WIDE, WIDE), WIDE)], w_s.at[0], w_sem.at[0])
    wv_copy = pltpu.make_async_copy(wv_ref.at[:, pl.ds(pl.multiple_of(c * WIDE, WIDE), WIDE)], w_s.at[1], w_sem.at[1])

    def wq_copy(i):
        first = pl.multiple_of((c * 4 + flip((i + 1) % 4 if isinstance(i, int) else lax.rem(i + 1, 4))) * WIDE, WIDE)
        return pltpu.make_async_copy(wq_ref.at[:, pl.ds(first, WIDE)], w_s.at[2 + i], w_sem.at[2 + i])

    def wo_start(k, core, slot):
        first = pl.multiple_of((core * 4 + flip(k)) * WIDE, WIDE)
        for j in range(tiles):
            pltpu.make_async_copy(wo_ref.at[pl.ds(first, WIDE), pl.ds(j * WIDE, WIDE)],
                                  w_s.at[slot, pl.ds(j * WIDE, WIDE), :], wo_sem.at[slot]).start()

    def wo_wait(slot):
        pltpu.make_async_copy(w_s.at[slot], w_s.at[slot], wo_sem.at[slot]).wait()

    x_copy.start()
    wk_copy.start()
    wv_copy.start()
    near_copy.start()
    far_copy.start()

    def clear(j, _):
        kv[j] = jnp.zeros((2 * ROWS, HEAD), jnp.bfloat16)

    lax.fori_loop(BLOCKS - 3, BLOCKS, clear, None)

    barrier = pltpu.get_barrier_semaphore()
    pl.semaphore_signal(barrier, inc=1, device_id=at(p, z, 1 - c), device_id_type=MESH)
    for k in (1, 2, 3):
        for core in (0, 1):
            pl.semaphore_signal(barrier, inc=1, device_id=at(flip(k), z, core), device_id_type=MESH)
    for step in (-1, 1):
        @pl.when((z + step >= 0) & (z + step <= 3))
        def _():
            pl.semaphore_signal(barrier, inc=1, device_id=at(p, z + step, c), device_id_type=MESH)
    pl.semaphore_wait(barrier, 8 + lax.div(z * (3 - z), 2))

    def x_piece(i, core):
        rows = pl.ds(i * (OWN // PIECES), OWN // PIECES)
        return send(xs.at[core, rows], xs.at[core, rows], xs_send.at[i], xs_recv.at[i], at(p, z, 1 - c))

    x_copy.wait()
    for i in range(PIECES):
        x_piece(i, c).start()
    wq_copy(0).start()

    def norm_rows(half, first, count):
        def rows(i, _):
            here = first + i * 16
            wide = xs[half, pl.ds(pl.multiple_of(here, 16), 16), :].astype(jnp.float32)
            scale = lax.rsqrt(jnp.mean(wide * wide, -1, keepdims=True) + 1e-6)
            gain = gain_ref[...].astype(jnp.float32)[None]
            a_s[pl.ds(pl.multiple_of(half * OWN + here, 16), 16), :] = (wide * scale * gain).astype(jnp.bfloat16)
        lax.fori_loop(0, count // 16, rows, None)

    norm_rows(c, 0, OWN)
    near_copy.wait()
    far_copy.wait()
    block_no = 4 * p + z
    base_cos, base_sin = far[0, pl.ds(block_no, 1), :], far[1, pl.ds(block_no, 1), :]
    turn[0] = near[0] * base_cos - near[1] * base_sin
    turn[1] = (near[1] * base_cos + near[0] * base_sin) * far[2, 0:1, :]

    def x_arrived(i, _):
        x_piece(i, 1 - c).wait_recv()
        norm_rows(1 - c, i * (OWN // PIECES), OWN // PIECES)

    lax.fori_loop(0, PIECES, x_arrived, None)

    def turned(t):
        t = t.astype(jnp.bfloat16).astype(jnp.float32)
        return (t * turn[0] + pltpu.roll(t, HEAD // 2, 1) * turn[1]).astype(jnp.bfloat16)

    wk_copy.wait()
    wv_copy.wait()
    wq_copy(1).start()
    wq_copy(2).start()
    wq_copy(3).start()

    def kvp(k):
        to = flip(k)
        return send(kvsend.at[to], kv.at[block_no], kvp_send.at[k - 1], kv_recv.at[block_no], at(to, z, c))

    def kv_arrival(block):
        return send(kv.at[block], kv.at[block], fwd_send.at[0], kv_recv.at[block], at(p, z, c))

    def along(k, act):
        from_ = flip(k)
        block = 4 * from_ + z
        for n, step in enumerate((1, -1)):
            ok = (z + step <= 3) if step > 0 else ((z + step >= 0) & (from_ < 3))

            @pl.when(ok)
            def _():
                act(send(kv.at[block], kv.at[block], kvz_send.at[2 * k + n], kv_recv.at[block], at(p, z + step, c)))

    def make_kv(i, _):
        j = px + i - 2 * px * i
        columns = pl.ds(pl.multiple_of(j * 2 * HEAD, 2 * HEAD), 2 * HEAD)
        k = _dot(a_s[...], w_s[0, :, columns])
        v = _dot(a_s[...], w_s[1, :, columns]).astype(jnp.bfloat16)
        for n in range(2):
            kvsend[2 * j + n, 0:ROWS, :] = turned(k[:, n * HEAD : (n + 1) * HEAD])
            flat = v[:, n * HEAD : (n + 1) * HEAD].T
            kvsend[2 * j + n, ROWS : ROWS + HEAD, :] = flat[:, :HEAD]
            kvsend[2 * j + n, ROWS + HEAD : 2 * ROWS, :] = flat[:, HEAD:]

        @pl.when(i == 0)
        def _():
            kv[block_no] = kvsend[p]
            kvp(1).start()
            along(0, lambda copy: copy.start())

    lax.fori_loop(0, 2, make_kv, None)
    kvp(2).start()
    kvp(3).start()

    def q_copy(i, to):
        return send(qsend.at[i], qall.at[p], q_send.at[i], q_recv.at[p], at(to, z, c))

    def make_q(i, _):
        wq_copy(i).wait()

        def part(j, _):
            columns = pl.ds(pl.multiple_of(j * 2 * HEAD, 2 * HEAD), 2 * HEAD)
            q = _dot(a_s[...], w_s[2 + i, :, columns])
            for n in range(2):
                qsend[i, 2 * j + n] = turned(q[:, n * HEAD : (n + 1) * HEAD])

        lax.fori_loop(0, 2, part, None)

        @pl.when(i < 3)
        def _():
            q_copy(i, flip(i + 1)).start()

        @pl.when(i > 0)
        def _():
            kv_arrival(4 * flip(i) + z).wait_recv()
            along(i, lambda copy: copy.start())

    lax.fori_loop(0, 4, make_q, None)
    qall[p] = qsend[3]
    for k in range(4):
        for n in range(2):
            core = c if n == 0 else 1 - c
            wo_start(k, core, 2 * k + n)

    for b in range(4):
        top_s[b] = jnp.full((1, COLS), -jnp.inf, jnp.float32)
        acc_s[b] = jnp.zeros((HEAD + 8, COLS), jnp.float32)

    e = HEAD**-0.5 * LOG2E
    strips = range(0, COLS, STRIP)

    def block(b, j0, j1, masked):
        keys = jnp.concatenate([kv[j, 0:ROWS, :] for j in (j0, j1)], axis=0)
        q = qall[b].reshape(COLS, HEAD)
        scores = [_dot(keys, q[n : n + STRIP, :], 1, 1) for n in strips]
        flat = jnp.concatenate([kv[j, n : n + HEAD, :] for j in (j0, j1) for n in (ROWS, ROWS + HEAD)], axis=1)
        values = jnp.concatenate([flat, jnp.ones((8, 2 * ROWS), jnp.bfloat16)], axis=0)
        if masked:
            gap = (lax.rem(lax.broadcasted_iota(jnp.int32, (ROWS, STRIP), 1), ROWS)
                   - lax.broadcasted_iota(jnp.int32, (ROWS, STRIP), 0))
            ok = jnp.concatenate([gap >= (j - (4 * b + z)) * ROWS for j in (j0, j1)], axis=0)
        weights, keeps = [], []
        for n, s in zip(strips, scores):
            if masked:
                s = jnp.where(ok, s, -jnp.inf)
            old = top_s[b, :, n : n + STRIP]
            top = jnp.maximum(old, s.max(axis=0, keepdims=True))
            top_s[b, :, n : n + STRIP] = top
            weights.append(jnp.exp2((s - top) * e).astype(jnp.bfloat16))
            keeps.append(jnp.exp2((old - top) * e))
        for n, w, keep in zip(strips, weights, keeps):
            acc_s[b, :, n : n + STRIP] = acc_s[b, :, n : n + STRIP] * keep + _dot(values, w)

    def unit(t):
        g, k = lax.div(t, 4), lax.rem(t, 4)
        inner = jnp.where(z == 1, jnp.where(g < 2, 1 - g, g), jnp.where(g < 2, 2 - g, 9 - 3 * g))
        zz = jnp.where(middle, inner, jnp.where(z == 0, g, 3 - g))
        pp = flip(k)
        return pp, zz, 4 * pp + zz

    def forward(t, act):
        pp, zz, j = unit(t)
        for step, ok in ((1, (zz < z) & (z < 3)), (-1, (zz > z) & (z > 0) & (pp < 3))):
            @pl.when(ok)
            def _():
                act(send(kv.at[j], kv.at[j], fwd_send.at[j], kv_recv.at[j], at(p, z + step, c)))

    def arrive(t):
        pp, zz, j = unit(t)

        @pl.when((zz <= z) | (pp < 3))
        def _():
            kv_arrival(j).wait_recv()

        forward(t, lambda copy: copy.start())

    def visit(k, kq, base):
        pp, z0, j0 = unit(base + k)
        _, z1, j1 = unit(base + k + 4)
        b = flip(kq)

        @pl.when(pp < b)
        def _():
            block(b, j0, j1, False)

        @pl.when((pp == b) & ((z0 <= z) | (z1 <= z)))
        def _():
            block(b, j0, j1, True)

    def q_arrive(k):
        q_from = flip(k)
        send(qall.at[q_from], qall.at[q_from], q_send.at[0], q_recv.at[q_from], at(p, z, c)).wait_recv()

    def attend(s, _):
        far_s = s - 16
        k = jnp.where(s < 16, lax.rem(s, 4), lax.div(far_s, 3))
        kq = jnp.where(s < 16, lax.div(s, 4), 1 + lax.rem(far_s + 15, 3))

        @pl.when(s < 4)
        def _():
            arrive(4 + s)

        @pl.when((s == 4) & middle)
        def _():
            lax.fori_loop(8, 12, lambda t, _: arrive(t), None)

        for n in (1, 2, 3):
            @pl.when(s == 4 * n)
            def _():
                q_arrive(n)

        @pl.when((s >= 16) & (kq == 1))
        def _():
            @pl.when((z == 0) | (z == 3))
            def _():
                arrive(8 + k)

            arrive(12 + k)

        visit(k, kq, jnp.where(s < 16, 0, 8))

    lax.fori_loop(0, 28, attend, None)

    def finish(b):
        total = acc_s[b, HEAD : HEAD + 1, :]
        return (acc_s[b, :HEAD, :] * (1 / total)).T.reshape(GROUP, 2, OWN, HEAD).astype(jnp.bfloat16)

    def o_copy(k, core):
        return send(osend.at[k, core], oall.at[p, c], o_send.at[k, core], o_recv.at[p, c], at(flip(k), z, core))

    def o_arrive(k, core):
        g = flip(k)
        send(oall.at[g, core], oall.at[g, core], o_send.at[0, 0], o_recv.at[g, core], at(p, z, c)).wait_recv()

    def finish_others(k, _):
        got = finish(flip(k))
        for core in range(2):
            osend[k, core] = got[:, core]
        for core in range(2):
            o_copy(k, core).start()

    lax.fori_loop(1, 4, finish_others, None)
    lax.fori_loop(0, 4, lambda k, _: visit(k, 0, 8), None)
    got = finish(p)
    osend[0, 1 - c] = jnp.where(c == 0, got[:, 1], got[:, 0])
    oall[p, c] = jnp.where(c == 0, got[:, 0], got[:, 1])
    o_copy(0, 1 - c).start()

    def heads(g, core):
        return jnp.concatenate([oall[g, core, n] for n in range(GROUP)], axis=1)

    def project(k, j, mine, other):
        rows = pl.ds(pl.multiple_of(j * WIDE, WIDE), WIDE)
        return _dot(mine, w_s[2 * k, rows, :]) + _dot(other, w_s[2 * k + 1, rows, :])

    def operands(k):
        @pl.when(k > 0)
        def _():
            o_arrive(k, c)

        o_arrive(k, 1 - c)
        wo_wait(2 * k)
        wo_wait(2 * k + 1)
        g = flip(k)
        return heads(g, c), heads(g, 1 - c)

    mine, other = operands(jnp.int32(0))

    def first_tile(j, _):
        columns = pl.ds(pl.multiple_of(j * WIDE, WIDE), WIDE)
        ysum[:, columns] = xs[c, :, columns].astype(jnp.float32) + project(0, j, mine, other)

    lax.fori_loop(0, tiles, first_tile, None)

    def middle_chips(k, _):
        mine, other = operands(k)

        def tile(j, _):
            columns = pl.ds(pl.multiple_of(j * WIDE, WIDE), WIDE)
            ysum[:, columns] = ysum[:, columns] + project(k, j, mine, other)

        lax.fori_loop(0, tiles, tile, None)

    lax.fori_loop(1, 3, middle_chips, None)
    mine3, other3 = operands(jnp.int32(3))

    def last_tile(j, _):
        columns = pl.ds(pl.multiple_of(j * WIDE, WIDE), WIDE)
        y_ref[:, columns] = (ysum[:, columns] + project(3, j, mine3, other3)).astype(jnp.bfloat16)

    lax.fori_loop(0, tiles, last_tile, None)

    for i in range(PIECES):
        x_piece(i, c).wait_send()
    for k in (1, 2, 3):
        kvp(k).wait_send()
        q_copy(k - 1, flip(k)).wait_send()
        for core in range(2):
            o_copy(k, core).wait_send()
    o_copy(0, 1 - c).wait_send()

    def sent(k, _):
        along(k, lambda copy: copy.wait_send())

    lax.fori_loop(0, 4, sent, None)
    lax.fori_loop(4, BLOCKS, lambda t, _: forward(t, lambda copy: copy.wait_send()), None)


def tables():
    half = HEAD // 2
    speed = np.tile(float(THETA) ** (-np.arange(half) / half), 2)
    near, far = np.arange(ROWS)[:, None] * speed, ROWS * np.arange(BLOCKS)[:, None] * speed
    sign = np.broadcast_to(np.where(np.arange(HEAD) < half, -1.0, 1.0), far.shape)
    return np.stack([np.cos(near), np.sin(near)]).astype(np.float32), np.stack([np.cos(far), np.sin(far), sign]).astype(np.float32)


def layer(x, gain, wq, wk, wv, wo):
    dim = x.shape[1]
    bf16, f32 = jnp.bfloat16, jnp.float32
    dma = pltpu.SemaphoreType.DMA
    vmem = pl.BlockSpec(memory_space=pltpu.VMEM)
    hbm = pl.BlockSpec(memory_space=pl.ANY)
    near, far = tables()
    return pl.pallas_call(
        _kernel,
        out_shape=pltpu.VMEM(x.shape, bf16),
        in_specs=[hbm, vmem, hbm, hbm, hbm, hbm, hbm, hbm],
        out_specs=vmem,
        scratch_shapes=[
            pltpu.VMEM((2, OWN, dim), bf16),
            pltpu.VMEM((ROWS, dim), bf16),
            pltpu.VMEM((8, dim, WIDE), bf16),
            pltpu.VMEM(near.shape, f32),
            pltpu.VMEM(far.shape, f32),
            pltpu.VMEM((2, ROWS, HEAD), f32),
            pltpu.VMEM((4, 2 * ROWS, HEAD), bf16),
            pltpu.VMEM((BLOCKS, 2 * ROWS, HEAD), bf16),
            pltpu.VMEM((4, GROUP, ROWS, HEAD), bf16),
            pltpu.VMEM((4, GROUP, ROWS, HEAD), bf16),
            pltpu.VMEM((4, 1, COLS), f32),
            pltpu.VMEM((4, HEAD + 8, COLS), f32),
            pltpu.VMEM((4, 2, GROUP, OWN, HEAD), bf16),
            pltpu.VMEM((4, 2, GROUP, OWN, HEAD), bf16),
            pltpu.VMEM((OWN, dim), f32),
            dma, dma((6,)), dma((8,)), dma((2,)), dma((PIECES,)), dma((PIECES,)), dma((3,)), dma((BLOCKS,)), dma((8,)), dma((BLOCKS,)),
            dma((3,)), dma((4,)), dma((4, 2)), dma((4, 2)),
        ],
        compiler_params=pltpu.CompilerParams(collective_id=0, has_side_effects=True, vmem_limit_bytes=61 * 2**20),
        cost_estimate=pl.CostEstimate(flops=20 * 10**9, bytes_accessed=80 * 10**6, transcendentals=10**7),
    )(x, gain, jnp.asarray(near), jnp.asarray(far), wq, wk, wv, wo)


def solution(mesh):
    def step(x, gain, wq, wk, wv, wo):
        return layer(x, gain, wq, wk, wv, wo)

    tokens, whole = P(("dp", "sp"), None), P(None, None)
    return jax.shard_map(
        step,
        mesh=mesh,
        in_specs=(tokens, P(None), whole, whole, whole, whole),
        out_specs=tokens,
        check_vma=False,
    )
```

```python
import numpy as np

import jax
import jax.numpy as jnp
from jax import lax
from jax.experimental import pallas as pl
from jax.experimental.pallas import tpu as pltpu
from jax.sharding import PartitionSpec as P

HEAD = 128
THETA = 10000
LOG2E = 1.4426950408889634
OWN = 128
ROWS = 256
BLOCKS = 16
GROUP = 4
WIDE = GROUP * HEAD
COLS = GROUP * ROWS
STRIP = 512
PIECES = 4
MESH = pl.DeviceIdType.MESH


def _dot(a, b, ca=1, cb=0):
    return lax.dot_general(a, b, (((ca,), (cb,)), ((), ())), preferred_element_type=jnp.float32)


def _kernel(x_ref, gain_ref, near_ref, far_ref, wq_ref, wk_ref, wv_ref, wo_ref, y_ref,
            xs, a_s, w_s, near, far, turn, kvsend, kv, qsend, qall, top_s, acc_s, osend, oall, ysum, ysend,
            x_sem, w_sem, wo_sem, t_sem, xs_send, xs_recv, kvp_send, kv_recv, kvz_send, fwd_send,
            q_send, q_recv, o_send, o_recv, p_send, y_send, y_recv):
    tiles = x_ref.shape[1] // (2 * WIDE)
    me = lax.axis_index("sp")
    c = lax.rem(me, 2)
    z = lax.rem(lax.div(me, 2), 4)
    p = lax.div(me, 8)
    px, py = lax.div(p, 2), lax.rem(p, 2)
    middle = (z == 1) | (z == 2)

    def flip(k):
        kx, ky = (k // 2, k % 2) if isinstance(k, int) else (lax.div(k, 2), lax.rem(k, 2))
        return 2 * (px + kx - 2 * px * kx) + (py + ky - 2 * py * ky)

    def at(p_, z_, c_):
        return {"sp": (p_ * 4 + z_) * 2 + c_}

    def send(src, dst, send_sem, recv_sem, device):
        return pltpu.make_async_remote_copy(src_ref=src, dst_ref=dst, send_sem=send_sem, recv_sem=recv_sem,
                                            device_id=device, device_id_type=MESH)

    x_copy = pltpu.make_async_copy(x_ref, xs.at[c], x_sem)
    near_copy = pltpu.make_async_copy(near_ref, near, t_sem.at[0])
    far_copy = pltpu.make_async_copy(far_ref, far, t_sem.at[1])
    wk_copy = pltpu.make_async_copy(wk_ref.at[:, pl.ds(pl.multiple_of(c * WIDE, WIDE), WIDE)], w_s.at[0], w_sem.at[0])
    wv_copy = pltpu.make_async_copy(wv_ref.at[:, pl.ds(pl.multiple_of(c * WIDE, WIDE), WIDE)], w_s.at[1], w_sem.at[1])

    def wq_copy(i):
        first = pl.multiple_of((c * 4 + flip((i + 1) % 4 if isinstance(i, int) else lax.rem(i + 1, 4))) * WIDE, WIDE)
        return pltpu.make_async_copy(wq_ref.at[:, pl.ds(first, WIDE)], w_s.at[2 + i], w_sem.at[2 + i])

    def wo_start(k):
        for n, core in enumerate((c, 1 - c)):
            rows = pl.ds(pl.multiple_of((core * 4 + flip(k)) * WIDE, WIDE), WIDE)
            for j in range(tiles):
                columns = pl.ds(pl.multiple_of((c * tiles + j) * WIDE, WIDE), WIDE)
                pltpu.make_async_copy(wo_ref.at[rows, columns], w_s.at[k, pl.ds((2 * j + n) * WIDE, WIDE), :], wo_sem.at[k]).start()

    def wo_wait(k):
        pltpu.make_async_copy(w_s.at[k], w_s.at[k], wo_sem.at[k]).wait()

    x_copy.start()
    wk_copy.start()
    wv_copy.start()
    near_copy.start()
    far_copy.start()

    def clear(j, _):
        kv[j] = jnp.zeros((2 * ROWS, HEAD), jnp.bfloat16)

    lax.fori_loop(BLOCKS - 3, BLOCKS, clear, None)

    barrier = pltpu.get_barrier_semaphore()
    pl.semaphore_signal(barrier, inc=1, device_id=at(p, z, 1 - c), device_id_type=MESH)
    for k in (1, 2, 3):
        pl.semaphore_signal(barrier, inc=1, device_id=at(flip(k), z, c), device_id_type=MESH)
    for step in (-1, 1):
        @pl.when((z + step >= 0) & (z + step <= 3))
        def _():
            pl.semaphore_signal(barrier, inc=1, device_id=at(p, z + step, c), device_id_type=MESH)
    pl.semaphore_wait(barrier, 5 + lax.div(z * (3 - z), 2))

    def x_piece(i, core):
        rows = pl.ds(i * (OWN // PIECES), OWN // PIECES)
        return send(xs.at[core, rows], xs.at[core, rows], xs_send.at[i], xs_recv.at[i], at(p, z, 1 - c))

    x_copy.wait()
    for i in range(PIECES):
        x_piece(i, c).start()
    wq_copy(0).start()

    def norm_rows(half, first, count):
        def rows(i, _):
            here = first + i * 16
            wide = xs[half, pl.ds(pl.multiple_of(here, 16), 16), :].astype(jnp.float32)
            scale = lax.rsqrt(jnp.mean(wide * wide, -1, keepdims=True) + 1e-6)
            gain = gain_ref[...].astype(jnp.float32)[None]
            a_s[pl.ds(pl.multiple_of(half * OWN + here, 16), 16), :] = (wide * scale * gain).astype(jnp.bfloat16)
        lax.fori_loop(0, count // 16, rows, None)

    norm_rows(c, 0, OWN)
    near_copy.wait()
    far_copy.wait()
    block_no = 4 * p + z
    base_cos, base_sin = far[0, pl.ds(block_no, 1), :], far[1, pl.ds(block_no, 1), :]
    turn[0] = near[0] * base_cos - near[1] * base_sin
    turn[1] = (near[1] * base_cos + near[0] * base_sin) * far[2, 0:1, :]

    def x_arrived(i, _):
        x_piece(i, 1 - c).wait_recv()
        norm_rows(1 - c, i * (OWN // PIECES), OWN // PIECES)

    lax.fori_loop(0, PIECES, x_arrived, None)

    def turned(t):
        t = t.astype(jnp.bfloat16).astype(jnp.float32)
        return (t * turn[0] + pltpu.roll(t, HEAD // 2, 1) * turn[1]).astype(jnp.bfloat16)

    wk_copy.wait()
    wv_copy.wait()
    wq_copy(1).start()
    wq_copy(2).start()
    wq_copy(3).start()

    def kvp(k):
        to = flip(k)
        return send(kvsend.at[to], kv.at[block_no], kvp_send.at[k - 1], kv_recv.at[block_no], at(to, z, c))

    def kv_arrival(block):
        return send(kv.at[block], kv.at[block], fwd_send.at[0], kv_recv.at[block], at(p, z, c))

    def along(k, act):
        from_ = flip(k)
        block = 4 * from_ + z
        for n, step in enumerate((1, -1)):
            ok = (z + step <= 3) if step > 0 else ((z + step >= 0) & (from_ < 3))

            @pl.when(ok)
            def _():
                act(send(kv.at[block], kv.at[block], kvz_send.at[2 * k + n], kv_recv.at[block], at(p, z + step, c)))

    def make_kv(i, _):
        j = px + i - 2 * px * i
        columns = pl.ds(pl.multiple_of(j * 2 * HEAD, 2 * HEAD), 2 * HEAD)
        k = _dot(a_s[...], w_s[0, :, columns])
        v = _dot(a_s[...], w_s[1, :, columns]).astype(jnp.bfloat16)
        for n in range(2):
            kvsend[2 * j + n, 0:ROWS, :] = turned(k[:, n * HEAD : (n + 1) * HEAD])
            flat = v[:, n * HEAD : (n + 1) * HEAD].T
            kvsend[2 * j + n, ROWS : ROWS + HEAD, :] = flat[:, :HEAD]
            kvsend[2 * j + n, ROWS + HEAD : 2 * ROWS, :] = flat[:, HEAD:]

        @pl.when(i == 0)
        def _():
            kv[block_no] = kvsend[p]
            kvp(1).start()
            along(0, lambda copy: copy.start())

    lax.fori_loop(0, 2, make_kv, None)
    kvp(2).start()
    kvp(3).start()

    def q_copy(i, to):
        return send(qsend.at[i], qall.at[p], q_send.at[i], q_recv.at[p], at(to, z, c))

    def make_q(i, _):
        wq_copy(i).wait()

        def part(j, _):
            columns = pl.ds(pl.multiple_of(j * 2 * HEAD, 2 * HEAD), 2 * HEAD)
            q = _dot(a_s[...], w_s[2 + i, :, columns])
            for n in range(2):
                qsend[i, 2 * j + n] = turned(q[:, n * HEAD : (n + 1) * HEAD])

        lax.fori_loop(0, 2, part, None)

        @pl.when(i < 3)
        def _():
            q_copy(i, flip(i + 1)).start()

        @pl.when(i > 0)
        def _():
            kv_arrival(4 * flip(i) + z).wait_recv()
            along(i, lambda copy: copy.start())

    lax.fori_loop(0, 4, make_q, None)
    qall[p] = qsend[3]
    for k in range(4):
        wo_start(k)

    for b in range(4):
        top_s[b] = jnp.full((1, COLS), -jnp.inf, jnp.float32)
        acc_s[b] = jnp.zeros((HEAD + 8, COLS), jnp.float32)

    e = HEAD**-0.5 * LOG2E
    strips = range(0, COLS, STRIP)

    def block(b, j0, j1, masked):
        keys = jnp.concatenate([kv[j, 0:ROWS, :] for j in (j0, j1)], axis=0)
        q = qall[b].reshape(COLS, HEAD)
        scores = [_dot(keys, q[n : n + STRIP, :], 1, 1) for n in strips]
        flat = jnp.concatenate([kv[j, n : n + HEAD, :] for j in (j0, j1) for n in (ROWS, ROWS + HEAD)], axis=1)
        values = jnp.concatenate([flat, jnp.ones((8, 2 * ROWS), jnp.bfloat16)], axis=0)
        if masked:
            gap = (lax.rem(lax.broadcasted_iota(jnp.int32, (ROWS, STRIP), 1), ROWS)
                   - lax.broadcasted_iota(jnp.int32, (ROWS, STRIP), 0))
            ok = jnp.concatenate([gap >= (j - (4 * b + z)) * ROWS for j in (j0, j1)], axis=0)
        weights, keeps = [], []
        for n, s in zip(strips, scores):
            if masked:
                s = jnp.where(ok, s, -jnp.inf)
            old = top_s[b, :, n : n + STRIP]
            top = jnp.maximum(old, s.max(axis=0, keepdims=True))
            top_s[b, :, n : n + STRIP] = top
            weights.append(jnp.exp2((s - top) * e).astype(jnp.bfloat16))
            keeps.append(jnp.exp2((old - top) * e))
        for n, w, keep in zip(strips, weights, keeps):
            acc_s[b, :, n : n + STRIP] = acc_s[b, :, n : n + STRIP] * keep + _dot(values, w)

    def unit(t):
        g, k = lax.div(t, 4), lax.rem(t, 4)
        inner = jnp.where(z == 1, jnp.where(g < 2, 1 - g, g), jnp.where(g < 2, 2 - g, 9 - 3 * g))
        zz = jnp.where(middle, inner, jnp.where(z == 0, g, 3 - g))
        pp = flip(k)
        return pp, zz, 4 * pp + zz

    def forward(t, act):
        pp, zz, j = unit(t)
        for step, ok in ((1, (zz < z) & (z < 3)), (-1, (zz > z) & (z > 0) & (pp < 3))):
            @pl.when(ok)
            def _():
                act(send(kv.at[j], kv.at[j], fwd_send.at[j], kv_recv.at[j], at(p, z + step, c)))

    def arrive(t):
        pp, zz, j = unit(t)

        @pl.when((zz <= z) | (pp < 3))
        def _():
            kv_arrival(j).wait_recv()

        forward(t, lambda copy: copy.start())

    def visit(k, kq, base):
        pp, z0, j0 = unit(base + k)
        _, z1, j1 = unit(base + k + 4)
        b = flip(kq)

        @pl.when(pp < b)
        def _():
            block(b, j0, j1, False)

        @pl.when((pp == b) & ((z0 <= z) | (z1 <= z)))
        def _():
            block(b, j0, j1, True)

    def q_arrive(k):
        q_from = flip(k)
        send(qall.at[q_from], qall.at[q_from], q_send.at[0], q_recv.at[q_from], at(p, z, c)).wait_recv()

    def finish(b):
        total = acc_s[b, HEAD : HEAD + 1, :]
        return (acc_s[b, :HEAD, :] * (1 / total)).T.reshape(GROUP, ROWS, HEAD).astype(jnp.bfloat16)

    def o_copy(k):
        return send(osend.at[k - 1], oall.at[p, c], o_send.at[k - 1], o_recv.at[p, c], at(flip(k), z, c))

    def attend(s, _):
        far_s = s - 16
        by_keys = z == 3
        k = jnp.where(s < 16, lax.rem(s, 4), jnp.where(by_keys, lax.div(far_s, 3), lax.rem(s, 4)))
        kq = jnp.where(s < 16, lax.div(s, 4), 1 + jnp.where(by_keys, lax.rem(far_s + 15, 3), lax.div(far_s, 4)))

        @pl.when(s < 4)
        def _():
            arrive(4 + s)

        @pl.when((s == 4) & middle)
        def _():
            lax.fori_loop(8, 12, lambda t, _: arrive(t), None)

        for n in (1, 2, 3):
            @pl.when(s == 4 * n)
            def _():
                q_arrive(n)

        @pl.when((s >= 16) & (kq == 1))
        def _():
            @pl.when((z == 0) | (z == 3))
            def _():
                arrive(8 + k)

            arrive(12 + k)

        visit(k, kq, jnp.where(s < 16, 0, 8))

        @pl.when((s >= 16) & (k == 3))
        def _():
            osend[kq - 1] = finish(flip(kq))
            o_copy(kq).start()

    lax.fori_loop(0, 28, attend, None)
    lax.fori_loop(0, 4, lambda k, _: visit(k, 0, 8), None)

    def pass_on(k):
        g = flip(k)
        return send(oall.at[g, c], oall.at[g, c], p_send.at[k], o_recv.at[g, c], at(p, z, 1 - c))

    def o_arrive(k, core):
        g = flip(k)
        send(oall.at[g, core], oall.at[g, core], o_send.at[0], o_recv.at[g, core], at(p, z, c)).wait_recv()

    def heads(g, core):
        return jnp.concatenate([oall[g, core, n] for n in range(GROUP)], axis=1)

    oall[p, c] = finish(p)

    def with_x(j, _):
        columns = pl.ds(pl.multiple_of((c * tiles + j) * WIDE, WIDE), WIDE)
        ysum[j] = xs[:, :, columns].reshape(ROWS, WIDE).astype(jnp.float32)

    lax.fori_loop(0, tiles, with_x, None)
    pass_on(0).start()

    def project(k, _):
        @pl.when(k > 0)
        def _():
            o_arrive(k, c)
            pass_on(k).start()

        wo_wait(k)
        o_arrive(k, 1 - c)
        g = flip(k)
        o = jnp.concatenate([heads(g, c), heads(g, 1 - c)], axis=1)

        def tile(j, _):
            ysum[j] = ysum[j] + _dot(o, w_s[k, pl.ds(pl.multiple_of(2 * j * WIDE, 2 * WIDE), 2 * WIDE), :])

        lax.fori_loop(0, tiles, tile, None)

    lax.fori_loop(0, 3, project, None)
    o_arrive(3, c)
    pass_on(3).start()
    wo_wait(3)
    mine = heads(flip(3), c)

    def half(j, _):
        ysum[j] = ysum[j] + _dot(mine, w_s[3, pl.ds(pl.multiple_of(2 * j * WIDE, WIDE), WIDE), :])

    lax.fori_loop(0, tiles, half, None)
    o_arrive(3, 1 - c)
    other = heads(flip(3), 1 - c)

    def y_copy(j, core):
        columns = pl.ds(pl.multiple_of((core * tiles + j) * WIDE, WIDE), WIDE)
        return send(ysend.at[j], y_ref.at[:, columns], y_send.at[j], y_recv.at[j], at(p, z, 1 - c))

    def last(j, _):
        got = ysum[j] + _dot(other, w_s[3, pl.ds(pl.multiple_of((2 * j + 1) * WIDE, WIDE), WIDE), :])
        got = got.astype(jnp.bfloat16)
        columns = pl.ds(pl.multiple_of((c * tiles + j) * WIDE, WIDE), WIDE)
        y_ref[:, columns] = jnp.where(c == 0, got[:OWN], got[OWN:])
        ysend[j] = jnp.where(c == 0, got[OWN:], got[:OWN])

        @pl.when(j > 0)
        def _():
            y_copy(j - 1, c).start()

    lax.fori_loop(0, tiles, last, None)
    y_copy(tiles - 1, c).start()
    lax.fori_loop(0, tiles, lambda j, _: y_copy(j, 1 - c).wait_recv(), None)

    for i in range(PIECES):
        x_piece(i, c).wait_send()
    for k in (1, 2, 3):
        kvp(k).wait_send()
        q_copy(k - 1, flip(k)).wait_send()
        o_copy(k).wait_send()
    for k in range(4):
        pass_on(k).wait_send()
    lax.fori_loop(0, tiles, lambda j, _: y_copy(j, c).wait_send(), None)

    def sent(k, _):
        along(k, lambda copy: copy.wait_send())

    lax.fori_loop(0, 4, sent, None)
    lax.fori_loop(4, BLOCKS, lambda t, _: forward(t, lambda copy: copy.wait_send()), None)


def tables():
    half = HEAD // 2
    speed = np.tile(float(THETA) ** (-np.arange(half) / half), 2)
    near, far = np.arange(ROWS)[:, None] * speed, ROWS * np.arange(BLOCKS)[:, None] * speed
    sign = np.broadcast_to(np.where(np.arange(HEAD) < half, -1.0, 1.0), far.shape)
    return np.stack([np.cos(near), np.sin(near)]).astype(np.float32), np.stack([np.cos(far), np.sin(far), sign]).astype(np.float32)


def layer(x, gain, wq, wk, wv, wo):
    dim = x.shape[1]
    tiles = dim // (2 * WIDE)
    bf16, f32 = jnp.bfloat16, jnp.float32
    dma = pltpu.SemaphoreType.DMA
    vmem = pl.BlockSpec(memory_space=pltpu.VMEM)
    hbm = pl.BlockSpec(memory_space=pl.ANY)
    near, far = tables()
    return pl.pallas_call(
        _kernel,
        out_shape=pltpu.VMEM(x.shape, bf16),
        in_specs=[hbm, vmem, hbm, hbm, hbm, hbm, hbm, hbm],
        out_specs=vmem,
        scratch_shapes=[
            pltpu.VMEM((2, OWN, dim), bf16),
            pltpu.VMEM((ROWS, dim), bf16),
            pltpu.VMEM((6, dim, WIDE), bf16),
            pltpu.VMEM(near.shape, f32),
            pltpu.VMEM(far.shape, f32),
            pltpu.VMEM((2, ROWS, HEAD), f32),
            pltpu.VMEM((4, 2 * ROWS, HEAD), bf16),
            pltpu.VMEM((BLOCKS, 2 * ROWS, HEAD), bf16),
            pltpu.VMEM((4, GROUP, ROWS, HEAD), bf16),
            pltpu.VMEM((4, GROUP, ROWS, HEAD), bf16),
            pltpu.VMEM((4, 1, COLS), f32),
            pltpu.VMEM((4, HEAD + 8, COLS), f32),
            pltpu.VMEM((3, GROUP, ROWS, HEAD), bf16),
            pltpu.VMEM((4, 2, GROUP, ROWS, HEAD), bf16),
            pltpu.VMEM((tiles, ROWS, WIDE), f32),
            pltpu.VMEM((tiles, OWN, WIDE), bf16),
            dma, dma((6,)), dma((4,)), dma((2,)), dma((PIECES,)), dma((PIECES,)), dma((3,)), dma((BLOCKS,)), dma((8,)), dma((BLOCKS,)),
            dma((3,)), dma((4,)), dma((3,)), dma((4, 2)), dma((4,)), dma((tiles,)), dma((tiles,)),
        ],
        compiler_params=pltpu.CompilerParams(collective_id=0, has_side_effects=True, vmem_limit_bytes=61 * 2**20),
        cost_estimate=pl.CostEstimate(flops=20 * 10**9, bytes_accessed=80 * 10**6, transcendentals=10**7),
    )(x, gain, jnp.asarray(near), jnp.asarray(far), wq, wk, wv, wo)


def solution(mesh):
    def step(x, gain, wq, wk, wv, wo):
        return layer(x, gain, wq, wk, wv, wo)

    tokens, whole = P(("dp", "sp"), None), P(None, None)
    return jax.shard_map(
        step,
        mesh=mesh,
        in_specs=(tokens, P(None), whole, whole, whole, whole),
        out_specs=tokens,
        check_vma=False,
    )
```

```python
import numpy as np

import jax
import jax.numpy as jnp
from jax import lax
from jax.experimental import pallas as pl
from jax.experimental.pallas import tpu as pltpu
from jax.sharding import PartitionSpec as P

HEAD = 128
THETA = 10000
LOG2E = 1.4426950408889634
OWN = 128
ROWS = 256
BLOCKS = 16
GROUP = 4
WIDE = GROUP * HEAD
COLS = GROUP * ROWS
STRIP = 512
PIECES = 4
MESH = pl.DeviceIdType.MESH


def _dot(a, b, ca=1, cb=0):
    return lax.dot_general(a, b, (((ca,), (cb,)), ((), ())), preferred_element_type=jnp.float32)


def _kernel(x_ref, gain_ref, near_ref, far_ref, wq_ref, wk_ref, wv_ref, wo_ref, y_ref,
            xs, a_s, w_s, near, far, turn, kvsend, kv, qsend, qall, top_s, acc_s, osend, oall, ysum, ysend,
            x_sem, w_sem, wo_sem, t_sem, xs_send, xs_recv, kvp_send, kv_recv, kvz_send, fwd_send,
            q_send, q_recv, o_send, o_recv, p_send, y_send, y_recv):
    tiles = x_ref.shape[1] // (2 * WIDE)
    me = lax.axis_index("sp")
    c = lax.rem(me, 2)
    z = lax.rem(lax.div(me, 2), 4)
    p = lax.div(me, 8)
    px, py = lax.div(p, 2), lax.rem(p, 2)
    middle = (z == 1) | (z == 2)

    def flip(k):
        kx, ky = (k // 2, k % 2) if isinstance(k, int) else (lax.div(k, 2), lax.rem(k, 2))
        return 2 * (px + kx - 2 * px * kx) + (py + ky - 2 * py * ky)

    def at(p_, z_, c_):
        return {"sp": (p_ * 4 + z_) * 2 + c_}

    def send(src, dst, send_sem, recv_sem, device):
        return pltpu.make_async_remote_copy(src_ref=src, dst_ref=dst, send_sem=send_sem, recv_sem=recv_sem,
                                            device_id=device, device_id_type=MESH)

    x_copy = pltpu.make_async_copy(x_ref, xs.at[c], x_sem)
    near_copy = pltpu.make_async_copy(near_ref, near, t_sem.at[0])
    far_copy = pltpu.make_async_copy(far_ref, far, t_sem.at[1])
    wk_copy = pltpu.make_async_copy(wk_ref.at[:, pl.ds(pl.multiple_of(c * WIDE, WIDE), WIDE)], w_s.at[0], w_sem.at[0])
    wv_copy = pltpu.make_async_copy(wv_ref.at[:, pl.ds(pl.multiple_of(c * WIDE, WIDE), WIDE)], w_s.at[1], w_sem.at[1])

    def wq_copy(i):
        first = pl.multiple_of((c * 4 + flip((i + 1) % 4 if isinstance(i, int) else lax.rem(i + 1, 4))) * WIDE, WIDE)
        return pltpu.make_async_copy(wq_ref.at[:, pl.ds(first, WIDE)], w_s.at[2 + i], w_sem.at[2 + i])

    def wo_start(k):
        for n, core in enumerate((c, 1 - c)):
            rows = pl.ds(pl.multiple_of((core * 4 + flip(k)) * WIDE, WIDE), WIDE)
            for j in range(tiles):
                columns = pl.ds(pl.multiple_of((c * tiles + j) * WIDE, WIDE), WIDE)
                pltpu.make_async_copy(wo_ref.at[rows, columns], w_s.at[k, pl.ds((2 * j + n) * WIDE, WIDE), :], wo_sem.at[k]).start()

    def wo_wait(k):
        pltpu.make_async_copy(w_s.at[k], w_s.at[k], wo_sem.at[k]).wait()

    x_copy.start()
    wk_copy.start()
    wv_copy.start()
    near_copy.start()
    far_copy.start()

    def clear(j, _):
        kv[j] = jnp.zeros((2 * ROWS, HEAD), jnp.bfloat16)

    lax.fori_loop(BLOCKS - 3, BLOCKS, clear, None)

    barrier = pltpu.get_barrier_semaphore()
    pl.semaphore_signal(barrier, inc=1, device_id=at(p, z, 1 - c), device_id_type=MESH)
    for k in (1, 2, 3):
        pl.semaphore_signal(barrier, inc=1, device_id=at(flip(k), z, c), device_id_type=MESH)
    for step in (-1, 1):
        @pl.when((z + step >= 0) & (z + step <= 3))
        def _():
            pl.semaphore_signal(barrier, inc=1, device_id=at(p, z + step, c), device_id_type=MESH)
    pl.semaphore_wait(barrier, 5 + lax.div(z * (3 - z), 2))

    def x_piece(i, core):
        rows = pl.ds(i * (OWN // PIECES), OWN // PIECES)
        return send(xs.at[core, rows], xs.at[core, rows], xs_send.at[i], xs_recv.at[i], at(p, z, 1 - c))

    x_copy.wait()
    for i in range(PIECES):
        x_piece(i, c).start()
    wq_copy(0).start()

    def norm_rows(half, first, count):
        def rows(i, _):
            here = first + i * 16
            wide = xs[half, pl.ds(pl.multiple_of(here, 16), 16), :].astype(jnp.float32)
            scale = lax.rsqrt(jnp.mean(wide * wide, -1, keepdims=True) + 1e-6)
            gain = gain_ref[...].astype(jnp.float32)[None]
            a_s[pl.ds(pl.multiple_of(half * OWN + here, 16), 16), :] = (wide * scale * gain).astype(jnp.bfloat16)
        lax.fori_loop(0, count // 16, rows, None)

    norm_rows(c, 0, OWN)
    near_copy.wait()
    far_copy.wait()
    block_no = 4 * p + z
    base_cos, base_sin = far[0, pl.ds(block_no, 1), :], far[1, pl.ds(block_no, 1), :]
    turn[0] = near[0] * base_cos - near[1] * base_sin
    turn[1] = (near[1] * base_cos + near[0] * base_sin) * far[2, 0:1, :]

    def x_arrived(i, _):
        x_piece(i, 1 - c).wait_recv()
        norm_rows(1 - c, i * (OWN // PIECES), OWN // PIECES)

    lax.fori_loop(0, PIECES, x_arrived, None)

    def turned(t):
        t = t.astype(jnp.bfloat16).astype(jnp.float32)
        return (t * turn[0] + pltpu.roll(t, HEAD // 2, 1) * turn[1]).astype(jnp.bfloat16)

    wk_copy.wait()
    wv_copy.wait()
    wq_copy(1).start()
    wq_copy(2).start()
    wq_copy(3).start()

    def kvp(k):
        to = flip(k)
        return send(kvsend.at[to], kv.at[block_no], kvp_send.at[k - 1], kv_recv.at[block_no], at(to, z, c))

    def kv_arrival(block):
        return send(kv.at[block], kv.at[block], fwd_send.at[0], kv_recv.at[block], at(p, z, c))

    def along(k, act):
        from_ = flip(k)
        block = 4 * from_ + z
        for n, step in enumerate((1, -1)):
            ok = (z + step <= 3) if step > 0 else ((z + step >= 0) & (from_ < 3))

            @pl.when(ok)
            def _():
                act(send(kv.at[block], kv.at[block], kvz_send.at[2 * k + n], kv_recv.at[block], at(p, z + step, c)))

    def make_kv(i, _):
        j = px + i - 2 * px * i
        columns = pl.ds(pl.multiple_of(j * 2 * HEAD, 2 * HEAD), 2 * HEAD)
        k = _dot(a_s[...], w_s[0, :, columns])
        v = _dot(a_s[...], w_s[1, :, columns]).astype(jnp.bfloat16)
        for n in range(2):
            kvsend[2 * j + n, 0:ROWS, :] = turned(k[:, n * HEAD : (n + 1) * HEAD])
            flat = v[:, n * HEAD : (n + 1) * HEAD].T
            kvsend[2 * j + n, ROWS : ROWS + HEAD, :] = flat[:, :HEAD]
            kvsend[2 * j + n, ROWS + HEAD : 2 * ROWS, :] = flat[:, HEAD:]

        @pl.when(i == 0)
        def _():
            kv[block_no] = kvsend[p]
            kvp(1).start()
            along(0, lambda copy: copy.start())

    lax.fori_loop(0, 2, make_kv, None)
    kvp(2).start()
    kvp(3).start()

    def q_copy(i, to):
        return send(qsend.at[i], qall.at[p], q_send.at[i], q_recv.at[p], at(to, z, c))

    def make_q(i, _):
        wq_copy(i).wait()

        def part(j, _):
            columns = pl.ds(pl.multiple_of(j * 2 * HEAD, 2 * HEAD), 2 * HEAD)
            q = _dot(a_s[...], w_s[2 + i, :, columns])
            for n in range(2):
                qsend[i, 2 * j + n] = turned(q[:, n * HEAD : (n + 1) * HEAD])

        lax.fori_loop(0, 2, part, None)

        @pl.when(i < 3)
        def _():
            q_copy(i, flip(i + 1)).start()

        @pl.when(i > 0)
        def _():
            kv_arrival(4 * flip(i) + z).wait_recv()
            along(i, lambda copy: copy.start())

    lax.fori_loop(0, 4, make_q, None)
    qall[p] = qsend[3]
    for k in range(4):
        wo_start(k)

    def with_x(j, _):
        columns = pl.ds(pl.multiple_of((c * tiles + j) * WIDE, WIDE), WIDE)
        ysum[j] = xs[:, :, columns].reshape(ROWS, WIDE).astype(jnp.float32)

    lax.fori_loop(0, tiles, with_x, None)

    for b in range(4):
        top_s[b] = jnp.full((1, COLS), -jnp.inf, jnp.float32)
        acc_s[b] = jnp.zeros((HEAD + 8, COLS), jnp.float32)

    e = HEAD**-0.5 * LOG2E
    strips = range(0, COLS, STRIP)

    def block(b, j0, j1, masked):
        keys = jnp.concatenate([kv[j, 0:ROWS, :] for j in (j0, j1)], axis=0)
        q = qall[b].reshape(COLS, HEAD)
        scores = [_dot(keys, q[n : n + STRIP, :], 1, 1) for n in strips]
        flat = jnp.concatenate([kv[j, n : n + HEAD, :] for j in (j0, j1) for n in (ROWS, ROWS + HEAD)], axis=1)
        values = jnp.concatenate([flat, jnp.ones((8, 2 * ROWS), jnp.bfloat16)], axis=0)
        if masked:
            gap = (lax.rem(lax.broadcasted_iota(jnp.int32, (ROWS, STRIP), 1), ROWS)
                   - lax.broadcasted_iota(jnp.int32, (ROWS, STRIP), 0))
            ok = jnp.concatenate([gap >= (j - (4 * b + z)) * ROWS for j in (j0, j1)], axis=0)
        weights, keeps = [], []
        for n, s in zip(strips, scores):
            if masked:
                s = jnp.where(ok, s, -jnp.inf)
            old = top_s[b, :, n : n + STRIP]
            top = jnp.maximum(old, s.max(axis=0, keepdims=True))
            top_s[b, :, n : n + STRIP] = top
            weights.append(jnp.exp2((s - top) * e).astype(jnp.bfloat16))
            keeps.append(jnp.exp2((old - top) * e))
        for n, w, keep in zip(strips, weights, keeps):
            acc_s[b, :, n : n + STRIP] = acc_s[b, :, n : n + STRIP] * keep + _dot(values, w)

    def unit(t):
        g, k = lax.div(t, 4), lax.rem(t, 4)
        inner = jnp.where(z == 1, jnp.where(g < 2, 1 - g, g), jnp.where(g < 2, 2 - g, 9 - 3 * g))
        zz = jnp.where(middle, inner, jnp.where(z == 0, g, 3 - g))
        pp = flip(k)
        return pp, zz, 4 * pp + zz

    def forward(t, act):
        pp, zz, j = unit(t)
        for step, ok in ((1, (zz < z) & (z < 3)), (-1, (zz > z) & (z > 0) & (pp < 3))):
            @pl.when(ok)
            def _():
                act(send(kv.at[j], kv.at[j], fwd_send.at[j], kv_recv.at[j], at(p, z + step, c)))

    def arrive(t):
        pp, zz, j = unit(t)

        @pl.when((zz <= z) | (pp < 3))
        def _():
            kv_arrival(j).wait_recv()

        forward(t, lambda copy: copy.start())

    def visit(k, kq, base):
        pp, z0, j0 = unit(base + k)
        _, z1, j1 = unit(base + k + 4)
        b = flip(kq)

        @pl.when(pp < b)
        def _():
            block(b, j0, j1, False)

        @pl.when((pp == b) & ((z0 <= z) | (z1 <= z)))
        def _():
            block(b, j0, j1, True)

    def q_arrive(k):
        q_from = flip(k)
        send(qall.at[q_from], qall.at[q_from], q_send.at[0], q_recv.at[q_from], at(p, z, c)).wait_recv()

    def finish(b):
        total = acc_s[b, HEAD : HEAD + 1, :]
        return (acc_s[b, :HEAD, :] * (1 / total)).T.reshape(GROUP, ROWS, HEAD).astype(jnp.bfloat16)

    def o_copy(k):
        return send(osend.at[k - 1], oall.at[p, c], o_send.at[k - 1], o_recv.at[p, c], at(flip(k), z, c))

    def attend(s, _):
        far_s = s - 16
        by_keys = z == 3
        k = jnp.where(s < 16, lax.rem(s, 4), jnp.where(by_keys, lax.div(far_s, 3), lax.rem(s, 4)))
        kq = jnp.where(s < 16, lax.div(s, 4), 1 + jnp.where(by_keys, lax.rem(far_s + 15, 3), lax.div(far_s, 4)))

        @pl.when(s < 4)
        def _():
            arrive(4 + s)

        @pl.when((s == 4) & middle)
        def _():
            lax.fori_loop(8, 12, lambda t, _: arrive(t), None)

        for n in (1, 2, 3):
            @pl.when(s == 4 * n)
            def _():
                q_arrive(n)

        @pl.when((s >= 16) & (kq == 1))
        def _():
            @pl.when((z == 0) | (z == 3))
            def _():
                arrive(8 + k)

            arrive(12 + k)

        visit(k, kq, jnp.where(s < 16, 0, 8))

        @pl.when((s >= 16) & (k == 3))
        def _():
            osend[kq - 1] = finish(flip(kq))
            o_copy(kq).start()

    lax.fori_loop(0, 28, attend, None)
    lax.fori_loop(0, 4, lambda k, _: visit(k, 0, 8), None)

    def pass_on(k):
        g = flip(k)
        return send(oall.at[g, c], oall.at[g, c], p_send.at[k], o_recv.at[g, c], at(p, z, 1 - c))

    def o_arrive(k, core):
        g = flip(k)
        send(oall.at[g, core], oall.at[g, core], o_send.at[0], o_recv.at[g, core], at(p, z, c)).wait_recv()

    def heads(g, core):
        return jnp.concatenate([oall[g, core, n] for n in range(GROUP)], axis=1)

    oall[p, c] = finish(p)

    pass_on(0).start()

    def part(j, k, n):
        return w_s[k, pl.ds(pl.multiple_of((2 * j + n) * WIDE, WIDE), WIDE), :]

    def add(k, core, n):
        o = heads(flip(k), core)

        def tile(j, _):
            ysum[j] = ysum[j] + _dot(o, part(j, k, n))

        lax.fori_loop(0, tiles, tile, None)

    wo_wait(0)
    add(0, c, 0)

    def project(k, _):
        o_arrive(k, c)
        pass_on(k).start()
        wo_wait(k)
        o_arrive(k - 1, 1 - c)
        mine, theirs = heads(flip(k), c), heads(flip(k - 1), 1 - c)

        def tile(j, _):
            ysum[j] = ysum[j] + (_dot(mine, part(j, k, 0)) + _dot(theirs, part(j, k - 1, 1)))

        lax.fori_loop(0, tiles, tile, None)

    lax.fori_loop(1, 3, project, None)
    o_arrive(2, 1 - c)
    add(2, 1 - c, 1)
    o_arrive(3, c)
    pass_on(3).start()
    wo_wait(3)
    add(3, c, 0)
    o_arrive(3, 1 - c)
    other = heads(flip(3), 1 - c)

    def y_copy(j, core):
        columns = pl.ds(pl.multiple_of((core * tiles + j) * WIDE, WIDE), WIDE)
        return send(ysend.at[j], y_ref.at[:, columns], y_send.at[j], y_recv.at[j], at(p, z, 1 - c))

    def last(j, _):
        got = ysum[j] + _dot(other, part(j, 3, 1))
        got = got.astype(jnp.bfloat16)
        columns = pl.ds(pl.multiple_of((c * tiles + j) * WIDE, WIDE), WIDE)
        y_ref[:, columns] = jnp.where(c == 0, got[:OWN], got[OWN:])
        ysend[j] = jnp.where(c == 0, got[OWN:], got[:OWN])

        @pl.when(j > 0)
        def _():
            y_copy(j - 1, c).start()

    lax.fori_loop(0, tiles, last, None)
    y_copy(tiles - 1, c).start()
    lax.fori_loop(0, tiles, lambda j, _: y_copy(j, 1 - c).wait_recv(), None)

    for i in range(PIECES):
        x_piece(i, c).wait_send()
    for k in (1, 2, 3):
        kvp(k).wait_send()
        q_copy(k - 1, flip(k)).wait_send()
        o_copy(k).wait_send()
    for k in range(4):
        pass_on(k).wait_send()
    lax.fori_loop(0, tiles, lambda j, _: y_copy(j, c).wait_send(), None)

    def sent(k, _):
        along(k, lambda copy: copy.wait_send())

    lax.fori_loop(0, 4, sent, None)
    lax.fori_loop(4, BLOCKS, lambda t, _: forward(t, lambda copy: copy.wait_send()), None)


def tables():
    half = HEAD // 2
    speed = np.tile(float(THETA) ** (-np.arange(half) / half), 2)
    near, far = np.arange(ROWS)[:, None] * speed, ROWS * np.arange(BLOCKS)[:, None] * speed
    sign = np.broadcast_to(np.where(np.arange(HEAD) < half, -1.0, 1.0), far.shape)
    return np.stack([np.cos(near), np.sin(near)]).astype(np.float32), np.stack([np.cos(far), np.sin(far), sign]).astype(np.float32)


def layer(x, gain, wq, wk, wv, wo):
    dim = x.shape[1]
    tiles = dim // (2 * WIDE)
    bf16, f32 = jnp.bfloat16, jnp.float32
    dma = pltpu.SemaphoreType.DMA
    vmem = pl.BlockSpec(memory_space=pltpu.VMEM)
    hbm = pl.BlockSpec(memory_space=pl.ANY)
    near, far = tables()
    return pl.pallas_call(
        _kernel,
        out_shape=pltpu.VMEM(x.shape, bf16),
        in_specs=[hbm, vmem, hbm, hbm, hbm, hbm, hbm, hbm],
        out_specs=vmem,
        scratch_shapes=[
            pltpu.VMEM((2, OWN, dim), bf16),
            pltpu.VMEM((ROWS, dim), bf16),
            pltpu.VMEM((6, dim, WIDE), bf16),
            pltpu.VMEM(near.shape, f32),
            pltpu.VMEM(far.shape, f32),
            pltpu.VMEM((2, ROWS, HEAD), f32),
            pltpu.VMEM((4, 2 * ROWS, HEAD), bf16),
            pltpu.VMEM((BLOCKS, 2 * ROWS, HEAD), bf16),
            pltpu.VMEM((4, GROUP, ROWS, HEAD), bf16),
            pltpu.VMEM((4, GROUP, ROWS, HEAD), bf16),
            pltpu.VMEM((4, 1, COLS), f32),
            pltpu.VMEM((4, HEAD + 8, COLS), f32),
            pltpu.VMEM((3, GROUP, ROWS, HEAD), bf16),
            pltpu.VMEM((4, 2, GROUP, ROWS, HEAD), bf16),
            pltpu.VMEM((tiles, ROWS, WIDE), f32),
            pltpu.VMEM((tiles, OWN, WIDE), bf16),
            dma, dma((6,)), dma((4,)), dma((2,)), dma((PIECES,)), dma((PIECES,)), dma((3,)), dma((BLOCKS,)), dma((8,)), dma((BLOCKS,)),
            dma((3,)), dma((4,)), dma((3,)), dma((4, 2)), dma((4,)), dma((tiles,)), dma((tiles,)),
        ],
        compiler_params=pltpu.CompilerParams(collective_id=0, has_side_effects=True, vmem_limit_bytes=61 * 2**20),
        cost_estimate=pl.CostEstimate(flops=20 * 10**9, bytes_accessed=80 * 10**6, transcendentals=10**7),
    )(x, gain, jnp.asarray(near), jnp.asarray(far), wq, wk, wv, wo)


def solution(mesh):
    def step(x, gain, wq, wk, wv, wo):
        return layer(x, gain, wq, wk, wv, wo)

    tokens, whole = P(("dp", "sp"), None), P(None, None)
    return jax.shard_map(
        step,
        mesh=mesh,
        in_specs=(tokens, P(None), whole, whole, whole, whole),
        out_specs=tokens,
        check_vma=False,
    )
```

```python
import numpy as np

import jax
import jax.numpy as jnp
from jax import lax
from jax.experimental import pallas as pl
from jax.experimental.pallas import tpu as pltpu
from jax.sharding import PartitionSpec as P

HEAD = 128
THETA = 10000
LOG2E = 1.4426950408889634
OWN = 128
ROWS = 256
BLOCKS = 16
GROUP = 4
WIDE = GROUP * HEAD
COLS = GROUP * ROWS
STRIP = 512
PIECES = 4
MESH = pl.DeviceIdType.MESH


def _dot(a, b, ca=1, cb=0):
    return lax.dot_general(a, b, (((ca,), (cb,)), ((), ())), preferred_element_type=jnp.float32)


def _kernel(x_ref, gain_ref, near_ref, far_ref, wq_ref, wk_ref, wv_ref, wo_ref, y_ref,
            xs, a_s, w_s, near, far, turn, kvsend, kv, qsend, qall, top_s, acc_s, osend, oall, ysum, ysend,
            x_sem, w_sem, wo_sem, t_sem, xs_send, xs_recv, kvp_send, kv_recv, kvz_send, fwd_send,
            q_send, q_recv, o_send, o_recv, p_send, y_send, y_recv):
    tiles = x_ref.shape[1] // (2 * WIDE)
    me = lax.axis_index("sp")
    c = lax.rem(me, 2)
    z = lax.rem(lax.div(me, 2), 4)
    p = lax.div(me, 8)
    px, py = lax.div(p, 2), lax.rem(p, 2)
    middle = (z == 1) | (z == 2)

    def flip(k):
        kx, ky = (k // 2, k % 2) if isinstance(k, int) else (lax.div(k, 2), lax.rem(k, 2))
        return 2 * (px + kx - 2 * px * kx) + (py + ky - 2 * py * ky)

    def at(p_, z_, c_):
        return {"sp": (p_ * 4 + z_) * 2 + c_}

    def send(src, dst, send_sem, recv_sem, device):
        return pltpu.make_async_remote_copy(src_ref=src, dst_ref=dst, send_sem=send_sem, recv_sem=recv_sem,
                                            device_id=device, device_id_type=MESH)

    x_copy = pltpu.make_async_copy(x_ref, xs.at[c], x_sem)
    near_copy = pltpu.make_async_copy(near_ref, near, t_sem.at[0])
    far_copy = pltpu.make_async_copy(far_ref, far, t_sem.at[1])
    wk_copy = pltpu.make_async_copy(wk_ref.at[:, pl.ds(pl.multiple_of(c * WIDE, WIDE), WIDE)], w_s.at[0], w_sem.at[0])
    wv_copy = pltpu.make_async_copy(wv_ref.at[:, pl.ds(pl.multiple_of(c * WIDE, WIDE), WIDE)], w_s.at[1], w_sem.at[1])

    def wq_copy(i):
        first = pl.multiple_of((c * 4 + flip((i + 1) % 4 if isinstance(i, int) else lax.rem(i + 1, 4))) * WIDE, WIDE)
        return pltpu.make_async_copy(wq_ref.at[:, pl.ds(first, WIDE)], w_s.at[2 + i], w_sem.at[2 + i])

    def wo_start(k):
        for n, core in enumerate((c, 1 - c)):
            rows = pl.ds(pl.multiple_of((core * 4 + flip(k)) * WIDE, WIDE), WIDE)
            for j in range(tiles):
                columns = pl.ds(pl.multiple_of((c * tiles + j) * WIDE, WIDE), WIDE)
                pltpu.make_async_copy(wo_ref.at[rows, columns], w_s.at[k, pl.ds((2 * j + n) * WIDE, WIDE), :], wo_sem.at[k]).start()

    def wo_wait(k):
        pltpu.make_async_copy(w_s.at[k], w_s.at[k], wo_sem.at[k]).wait()

    x_copy.start()
    wk_copy.start()
    wv_copy.start()
    near_copy.start()
    far_copy.start()

    def clear(j, _):
        kv[j] = jnp.zeros((2 * ROWS, HEAD), jnp.bfloat16)

    lax.fori_loop(BLOCKS - 3, BLOCKS, clear, None)

    barrier = pltpu.get_barrier_semaphore()
    pl.semaphore_signal(barrier, inc=1, device_id=at(p, z, 1 - c), device_id_type=MESH)
    for k in (1, 2, 3):
        pl.semaphore_signal(barrier, inc=1, device_id=at(flip(k), z, c), device_id_type=MESH)
    for step in (-1, 1):
        @pl.when((z + step >= 0) & (z + step <= 3))
        def _():
            pl.semaphore_signal(barrier, inc=1, device_id=at(p, z + step, c), device_id_type=MESH)
    pl.semaphore_wait(barrier, 5 + lax.div(z * (3 - z), 2))

    def x_piece(i, core):
        rows = pl.ds(i * (OWN // PIECES), OWN // PIECES)
        return send(xs.at[core, rows], xs.at[core, rows], xs_send.at[i], xs_recv.at[i], at(p, z, 1 - c))

    x_copy.wait()
    for i in range(PIECES):
        x_piece(i, c).start()
    wq_copy(0).start()

    def norm_rows(half, first, count):
        def rows(i, _):
            here = first + i * 16
            wide = xs[half, pl.ds(pl.multiple_of(here, 16), 16), :].astype(jnp.float32)
            scale = lax.rsqrt(jnp.mean(wide * wide, -1, keepdims=True) + 1e-6)
            gain = gain_ref[...].astype(jnp.float32)[None]
            a_s[pl.ds(pl.multiple_of(half * OWN + here, 16), 16), :] = (wide * scale * gain).astype(jnp.bfloat16)
        lax.fori_loop(0, count // 16, rows, None)

    norm_rows(c, 0, OWN)
    near_copy.wait()
    far_copy.wait()
    block_no = 4 * p + z
    base_cos, base_sin = far[0, pl.ds(block_no, 1), :], far[1, pl.ds(block_no, 1), :]
    turn[0] = near[0] * base_cos - near[1] * base_sin
    turn[1] = (near[1] * base_cos + near[0] * base_sin) * far[2, 0:1, :]

    def x_arrived(i, _):
        x_piece(i, 1 - c).wait_recv()
        norm_rows(1 - c, i * (OWN // PIECES), OWN // PIECES)

    lax.fori_loop(0, PIECES, x_arrived, None)

    def turned(t):
        t = t.astype(jnp.bfloat16).astype(jnp.float32)
        return (t * turn[0] + pltpu.roll(t, HEAD // 2, 1) * turn[1]).astype(jnp.bfloat16)

    wk_copy.wait()
    wv_copy.wait()
    wq_copy(1).start()
    wq_copy(2).start()
    wq_copy(3).start()

    def kvp(k):
        to = flip(k)
        return send(kvsend.at[to], kv.at[block_no], kvp_send.at[k - 1], kv_recv.at[block_no], at(to, z, c))

    def kv_arrival(block):
        return send(kv.at[block], kv.at[block], fwd_send.at[0], kv_recv.at[block], at(p, z, c))

    def along(k, act):
        from_ = flip(k)
        block = 4 * from_ + z
        for n, step in enumerate((1, -1)):
            ok = (z + step <= 3) if step > 0 else ((z + step >= 0) & (from_ < 3))

            @pl.when(ok)
            def _():
                act(send(kv.at[block], kv.at[block], kvz_send.at[2 * k + n], kv_recv.at[block], at(p, z + step, c)))

    def make_kv(i, _):
        j = px + i - 2 * px * i
        columns = pl.ds(pl.multiple_of(j * 2 * HEAD, 2 * HEAD), 2 * HEAD)
        k = _dot(a_s[...], w_s[0, :, columns])
        v = _dot(a_s[...], w_s[1, :, columns]).astype(jnp.bfloat16)
        for n in range(2):
            kvsend[2 * j + n, 0:ROWS, :] = turned(k[:, n * HEAD : (n + 1) * HEAD])
            flat = v[:, n * HEAD : (n + 1) * HEAD].T
            kvsend[2 * j + n, ROWS : ROWS + HEAD, :] = flat[:, :HEAD]
            kvsend[2 * j + n, ROWS + HEAD : 2 * ROWS, :] = flat[:, HEAD:]

        @pl.when(i == 0)
        def _():
            kv[block_no] = kvsend[p]
            kvp(1).start()
            along(0, lambda copy: copy.start())

    lax.fori_loop(0, 2, make_kv, None)
    kvp(2).start()
    kvp(3).start()

    def q_copy(i, to):
        return send(qsend.at[i], qall.at[p], q_send.at[i], q_recv.at[p], at(to, z, c))

    def make_q(i, _):
        wq_copy(i).wait()

        def part(j, _):
            columns = pl.ds(pl.multiple_of(j * 2 * HEAD, 2 * HEAD), 2 * HEAD)
            q = _dot(a_s[...], w_s[2 + i, :, columns])
            for n in range(2):
                qsend[i, 2 * j + n] = turned(q[:, n * HEAD : (n + 1) * HEAD])

        lax.fori_loop(0, 2, part, None)

        @pl.when(i < 3)
        def _():
            q_copy(i, flip(i + 1)).start()

        @pl.when(i > 0)
        def _():
            kv_arrival(4 * flip(i) + z).wait_recv()
            along(i, lambda copy: copy.start())

    lax.fori_loop(0, 4, make_q, None)
    qall[p] = qsend[3]
    for k in range(4):
        wo_start(k)

    def with_x(j, _):
        columns = pl.ds(pl.multiple_of((c * tiles + j) * WIDE, WIDE), WIDE)
        ysum[j] = xs[:, :, columns].reshape(ROWS, WIDE).astype(jnp.float32)

    lax.fori_loop(0, tiles, with_x, None)

    for b in range(4):
        top_s[b] = jnp.full((1, COLS), -jnp.inf, jnp.float32)
        acc_s[b] = jnp.zeros((HEAD + 8, COLS), jnp.float32)

    e = HEAD**-0.5 * LOG2E
    strips = range(0, COLS, STRIP)

    def block(b, j0, j1, masked):
        keys = jnp.concatenate([kv[j, 0:ROWS, :] for j in (j0, j1)], axis=0)
        q = qall[b].reshape(COLS, HEAD)
        scores = [_dot(keys, q[n : n + STRIP, :], 1, 1) for n in strips]
        flat = jnp.concatenate([kv[j, n : n + HEAD, :] for j in (j0, j1) for n in (ROWS, ROWS + HEAD)], axis=1)
        values = jnp.concatenate([flat, jnp.ones((8, 2 * ROWS), jnp.bfloat16)], axis=0)
        if masked:
            gap = (lax.rem(lax.broadcasted_iota(jnp.int32, (ROWS, STRIP), 1), ROWS)
                   - lax.broadcasted_iota(jnp.int32, (ROWS, STRIP), 0))
            ok = jnp.concatenate([gap >= (j - (4 * b + z)) * ROWS for j in (j0, j1)], axis=0)
        weights, keeps = [], []
        for n, s in zip(strips, scores):
            if masked:
                s = jnp.where(ok, s, -jnp.inf)
            old = top_s[b, :, n : n + STRIP]
            top = jnp.maximum(old, s.max(axis=0, keepdims=True))
            top_s[b, :, n : n + STRIP] = top
            weights.append(jnp.exp2((s - top) * e).astype(jnp.bfloat16))
            keeps.append(jnp.exp2((old - top) * e))
        for n, w, keep in zip(strips, weights, keeps):
            acc_s[b, :, n : n + STRIP] = acc_s[b, :, n : n + STRIP] * keep + _dot(values, w)

    def unit(t):
        g, k = lax.div(t, 4), lax.rem(t, 4)
        inner = jnp.where(z == 1, jnp.where(g < 2, 1 - g, g), jnp.where(g < 2, 2 - g, 9 - 3 * g))
        zz = jnp.where(middle, inner, jnp.where(z == 0, g, 3 - g))
        pp = flip(k)
        return pp, zz, 4 * pp + zz

    def forward(t, act):
        pp, zz, j = unit(t)
        for step, ok in ((1, (zz < z) & (z < 3)), (-1, (zz > z) & (z > 0) & (pp < 3))):
            @pl.when(ok)
            def _():
                act(send(kv.at[j], kv.at[j], fwd_send.at[j], kv_recv.at[j], at(p, z + step, c)))

    def arrive(t):
        pp, zz, j = unit(t)

        @pl.when((zz <= z) | (pp < 3))
        def _():
            kv_arrival(j).wait_recv()

        forward(t, lambda copy: copy.start())

    def visit(k, kq, base):
        pp, z0, j0 = unit(base + k)
        _, z1, j1 = unit(base + k + 4)
        b = flip(kq)

        @pl.when(pp < b)
        def _():
            block(b, j0, j1, False)

        @pl.when((pp == b) & ((z0 <= z) | (z1 <= z)))
        def _():
            block(b, j0, j1, True)

    def q_arrive(k):
        q_from = flip(k)
        send(qall.at[q_from], qall.at[q_from], q_send.at[0], q_recv.at[q_from], at(p, z, c)).wait_recv()

    def finish(b):
        total = acc_s[b, HEAD : HEAD + 1, :]
        return (acc_s[b, :HEAD, :] * (1 / total)).T.reshape(GROUP, ROWS, HEAD).astype(jnp.bfloat16)

    def o_copy(k):
        return send(osend.at[k - 1], oall.at[p, c], o_send.at[k - 1], o_recv.at[p, c], at(flip(k), z, c))

    def attend(s, _):
        k, turn_no = lax.rem(s, 4), lax.div(s, 4)
        kq = jnp.where(s < 16, turn_no, jnp.where(s < 20, 3, turn_no - 4))

        @pl.when(s < 4)
        def _():
            arrive(4 + s)

        @pl.when((s == 4) & middle)
        def _():
            lax.fori_loop(8, 12, lambda t, _: arrive(t), None)

        for n in (1, 2, 3):
            @pl.when(s == 4 * n)
            def _():
                q_arrive(n)

        @pl.when((s >= 16) & (s < 20))
        def _():
            @pl.when((z == 0) | (z == 3))
            def _():
                arrive(8 + k)

            arrive(12 + k)

        visit(k, kq, jnp.where(s < 16, 0, 8))

        @pl.when((s >= 16) & (k == 3))
        def _():
            osend[kq - 1] = finish(flip(kq))
            o_copy(kq).start()

    lax.fori_loop(0, 28, attend, None)
    lax.fori_loop(0, 4, lambda k, _: visit(k, 0, 8), None)

    def pass_on(k):
        g = flip(k)
        return send(oall.at[g, c], oall.at[g, c], p_send.at[k], o_recv.at[g, c], at(p, z, 1 - c))

    def o_arrive(k, core):
        g = flip(k)
        send(oall.at[g, core], oall.at[g, core], o_send.at[0], o_recv.at[g, core], at(p, z, c)).wait_recv()

    def heads(g, core):
        return jnp.concatenate([oall[g, core, n] for n in range(GROUP)], axis=1)

    oall[p, c] = finish(p)

    pass_on(0).start()

    def part(j, k, n):
        return w_s[k, pl.ds(pl.multiple_of((2 * j + n) * WIDE, WIDE), WIDE), :]

    def add(k, core, n):
        o = heads(flip(k), core)

        def tile(j, _):
            ysum[j] = ysum[j] + _dot(o, part(j, k, n))

        lax.fori_loop(0, tiles, tile, None)

    wo_wait(0)
    add(0, c, 0)

    def project(k, before):
        o_arrive(k, c)
        pass_on(k).start()
        wo_wait(k)
        o_arrive(before, 1 - c)
        mine, theirs = heads(flip(k), c), heads(flip(before), 1 - c)

        def tile(j, _):
            ysum[j] = ysum[j] + (_dot(mine, part(j, k, 0)) + _dot(theirs, part(j, before, 1)))

        lax.fori_loop(0, tiles, tile, None)

    project(3, 0)
    project(1, 3)
    o_arrive(1, 1 - c)
    add(1, 1 - c, 1)
    o_arrive(2, c)
    pass_on(2).start()
    wo_wait(2)
    add(2, c, 0)
    o_arrive(2, 1 - c)
    other = heads(flip(2), 1 - c)

    def y_copy(j, core):
        columns = pl.ds(pl.multiple_of((core * tiles + j) * WIDE, WIDE), WIDE)
        return send(ysend.at[j], y_ref.at[:, columns], y_send.at[j], y_recv.at[j], at(p, z, 1 - c))

    def last(j, _):
        got = ysum[j] + _dot(other, part(j, 2, 1))
        got = got.astype(jnp.bfloat16)
        columns = pl.ds(pl.multiple_of((c * tiles + j) * WIDE, WIDE), WIDE)
        y_ref[:, columns] = jnp.where(c == 0, got[:OWN], got[OWN:])
        ysend[j] = jnp.where(c == 0, got[OWN:], got[:OWN])

        @pl.when(j > 0)
        def _():
            y_copy(j - 1, c).start()

    lax.fori_loop(0, tiles, last, None)
    y_copy(tiles - 1, c).start()
    lax.fori_loop(0, tiles, lambda j, _: y_copy(j, 1 - c).wait_recv(), None)

    for i in range(PIECES):
        x_piece(i, c).wait_send()
    for k in (1, 2, 3):
        kvp(k).wait_send()
        q_copy(k - 1, flip(k)).wait_send()
        o_copy(k).wait_send()
    for k in range(4):
        pass_on(k).wait_send()
    lax.fori_loop(0, tiles, lambda j, _: y_copy(j, c).wait_send(), None)

    def sent(k, _):
        along(k, lambda copy: copy.wait_send())

    lax.fori_loop(0, 4, sent, None)
    lax.fori_loop(4, BLOCKS, lambda t, _: forward(t, lambda copy: copy.wait_send()), None)


def tables():
    half = HEAD // 2
    speed = np.tile(float(THETA) ** (-np.arange(half) / half), 2)
    near, far = np.arange(ROWS)[:, None] * speed, ROWS * np.arange(BLOCKS)[:, None] * speed
    sign = np.broadcast_to(np.where(np.arange(HEAD) < half, -1.0, 1.0), far.shape)
    return np.stack([np.cos(near), np.sin(near)]).astype(np.float32), np.stack([np.cos(far), np.sin(far), sign]).astype(np.float32)


def layer(x, gain, wq, wk, wv, wo):
    dim = x.shape[1]
    tiles = dim // (2 * WIDE)
    bf16, f32 = jnp.bfloat16, jnp.float32
    dma = pltpu.SemaphoreType.DMA
    vmem = pl.BlockSpec(memory_space=pltpu.VMEM)
    hbm = pl.BlockSpec(memory_space=pl.ANY)
    near, far = tables()
    return pl.pallas_call(
        _kernel,
        out_shape=pltpu.VMEM(x.shape, bf16),
        in_specs=[hbm, vmem, hbm, hbm, hbm, hbm, hbm, hbm],
        out_specs=vmem,
        scratch_shapes=[
            pltpu.VMEM((2, OWN, dim), bf16),
            pltpu.VMEM((ROWS, dim), bf16),
            pltpu.VMEM((6, dim, WIDE), bf16),
            pltpu.VMEM(near.shape, f32),
            pltpu.VMEM(far.shape, f32),
            pltpu.VMEM((2, ROWS, HEAD), f32),
            pltpu.VMEM((4, 2 * ROWS, HEAD), bf16),
            pltpu.VMEM((BLOCKS, 2 * ROWS, HEAD), bf16),
            pltpu.VMEM((4, GROUP, ROWS, HEAD), bf16),
            pltpu.VMEM((4, GROUP, ROWS, HEAD), bf16),
            pltpu.VMEM((4, 1, COLS), f32),
            pltpu.VMEM((4, HEAD + 8, COLS), f32),
            pltpu.VMEM((3, GROUP, ROWS, HEAD), bf16),
            pltpu.VMEM((4, 2, GROUP, ROWS, HEAD), bf16),
            pltpu.VMEM((tiles, ROWS, WIDE), f32),
            pltpu.VMEM((tiles, OWN, WIDE), bf16),
            dma, dma((6,)), dma((4,)), dma((2,)), dma((PIECES,)), dma((PIECES,)), dma((3,)), dma((BLOCKS,)), dma((8,)), dma((BLOCKS,)),
            dma((3,)), dma((4,)), dma((3,)), dma((4, 2)), dma((4,)), dma((tiles,)), dma((tiles,)),
        ],
        compiler_params=pltpu.CompilerParams(collective_id=0, has_side_effects=True, vmem_limit_bytes=61 * 2**20),
        cost_estimate=pl.CostEstimate(flops=20 * 10**9, bytes_accessed=80 * 10**6, transcendentals=10**7),
    )(x, gain, jnp.asarray(near), jnp.asarray(far), wq, wk, wv, wo)


def solution(mesh):
    def step(x, gain, wq, wk, wv, wo):
        return layer(x, gain, wq, wk, wv, wo)

    tokens, whole = P(("dp", "sp"), None), P(None, None)
    return jax.shard_map(
        step,
        mesh=mesh,
        in_specs=(tokens, P(None), whole, whole, whole, whole),
        out_specs=tokens,
        check_vma=False,
    )
```

```python
import numpy as np

import jax
import jax.numpy as jnp
from jax import lax
from jax.experimental import pallas as pl
from jax.experimental.pallas import tpu as pltpu
from jax.sharding import PartitionSpec as P

HEAD = 128
THETA = 10000
LOG2E = 1.4426950408889634
OWN = 128
ROWS = 256
BLOCKS = 16
GROUP = 4
WIDE = GROUP * HEAD
COLS = GROUP * ROWS
STRIP = 512
PIECES = 4
MESH = pl.DeviceIdType.MESH


def _dot(a, b, ca=1, cb=0):
    return lax.dot_general(a, b, (((ca,), (cb,)), ((), ())), preferred_element_type=jnp.float32)


def _kernel(x_ref, gain_ref, near_ref, far_ref, wq_ref, wk_ref, wv_ref, wo_ref, y_ref,
            xs, a_s, w_s, near, far, turn, kvsend, kv, qsend, qall, top_s, acc_s, osend, oall, ysum, ysend,
            x_sem, w_sem, wo_sem, t_sem, xs_send, xs_recv, kvp_send, kv_recv, kvz_send, fwd_send,
            q_send, q_recv, o_send, o_recv, p_send, y_send, y_recv):
    tiles = x_ref.shape[1] // (2 * WIDE)
    me = lax.axis_index("sp")
    c = lax.rem(me, 2)
    z = lax.rem(lax.div(me, 2), 4)
    p = lax.div(me, 8)
    px, py = lax.div(p, 2), lax.rem(p, 2)
    middle = (z == 1) | (z == 2)

    def flip(k):
        kx, ky = (k // 2, k % 2) if isinstance(k, int) else (lax.div(k, 2), lax.rem(k, 2))
        return 2 * (px + kx - 2 * px * kx) + (py + ky - 2 * py * ky)

    def at(p_, z_, c_):
        return {"sp": (p_ * 4 + z_) * 2 + c_}

    def send(src, dst, send_sem, recv_sem, device):
        return pltpu.make_async_remote_copy(src_ref=src, dst_ref=dst, send_sem=send_sem, recv_sem=recv_sem,
                                            device_id=device, device_id_type=MESH)

    x_copy = pltpu.make_async_copy(x_ref, xs.at[c], x_sem)
    near_copy = pltpu.make_async_copy(near_ref, near, t_sem.at[0])
    far_copy = pltpu.make_async_copy(far_ref, far, t_sem.at[1])
    wk_copy = pltpu.make_async_copy(wk_ref.at[:, pl.ds(pl.multiple_of(c * WIDE, WIDE), WIDE)], w_s.at[0], w_sem.at[0])
    wv_copy = pltpu.make_async_copy(wv_ref.at[:, pl.ds(pl.multiple_of(c * WIDE, WIDE), WIDE)], w_s.at[1], w_sem.at[1])

    def wq_copy(i):
        first = pl.multiple_of((c * 4 + flip((i + 1) % 4 if isinstance(i, int) else lax.rem(i + 1, 4))) * WIDE, WIDE)
        return pltpu.make_async_copy(wq_ref.at[:, pl.ds(first, WIDE)], w_s.at[2 + i], w_sem.at[2 + i])

    def wo_start(k):
        for n, core in enumerate((c, 1 - c)):
            rows = pl.ds(pl.multiple_of((core * 4 + flip(k)) * WIDE, WIDE), WIDE)
            for j in range(tiles):
                columns = pl.ds(pl.multiple_of((c * tiles + j) * WIDE, WIDE), WIDE)
                pltpu.make_async_copy(wo_ref.at[rows, columns], w_s.at[k, pl.ds((2 * j + n) * WIDE, WIDE), :], wo_sem.at[k]).start()

    def wo_wait(k):
        pltpu.make_async_copy(w_s.at[k], w_s.at[k], wo_sem.at[k]).wait()

    x_copy.start()
    wk_copy.start()
    wv_copy.start()
    near_copy.start()
    far_copy.start()

    def clear(j, _):
        kv[j] = jnp.zeros((2 * ROWS, HEAD), jnp.bfloat16)

    lax.fori_loop(BLOCKS - 3, BLOCKS, clear, None)

    barrier = pltpu.get_barrier_semaphore()
    pl.semaphore_signal(barrier, inc=1, device_id=at(p, z, 1 - c), device_id_type=MESH)
    for k in (1, 2, 3):
        pl.semaphore_signal(barrier, inc=1, device_id=at(flip(k), z, c), device_id_type=MESH)
    for step in (-1, 1):
        @pl.when((z + step >= 0) & (z + step <= 3))
        def _():
            pl.semaphore_signal(barrier, inc=1, device_id=at(p, z + step, c), device_id_type=MESH)
    pl.semaphore_wait(barrier, 5 + lax.div(z * (3 - z), 2))

    def x_piece(i, core):
        rows = pl.ds(i * (OWN // PIECES), OWN // PIECES)
        return send(xs.at[core, rows], xs.at[core, rows], xs_send.at[i], xs_recv.at[i], at(p, z, 1 - c))

    x_copy.wait()
    for i in range(PIECES):
        x_piece(i, c).start()
    wq_copy(0).start()

    def norm_rows(half, first, count):
        def rows(i, _):
            here = first + i * 16
            wide = xs[half, pl.ds(pl.multiple_of(here, 16), 16), :].astype(jnp.float32)
            scale = lax.rsqrt(jnp.mean(wide * wide, -1, keepdims=True) + 1e-6)
            gain = gain_ref[...].astype(jnp.float32)[None]
            a_s[pl.ds(pl.multiple_of(half * OWN + here, 16), 16), :] = (wide * scale * gain).astype(jnp.bfloat16)
        lax.fori_loop(0, count // 16, rows, None)

    norm_rows(c, 0, OWN)
    near_copy.wait()
    far_copy.wait()
    block_no = 4 * p + z
    base_cos, base_sin = far[0, pl.ds(block_no, 1), :], far[1, pl.ds(block_no, 1), :]
    turn[0] = near[0] * base_cos - near[1] * base_sin
    turn[1] = (near[1] * base_cos + near[0] * base_sin) * far[2, 0:1, :]

    def x_arrived(i, _):
        x_piece(i, 1 - c).wait_recv()
        norm_rows(1 - c, i * (OWN // PIECES), OWN // PIECES)

    lax.fori_loop(0, PIECES, x_arrived, None)

    def turned(t):
        t = t.astype(jnp.bfloat16).astype(jnp.float32)
        return (t * turn[0] + pltpu.roll(t, HEAD // 2, 1) * turn[1]).astype(jnp.bfloat16)

    wk_copy.wait()
    wv_copy.wait()
    wq_copy(1).start()
    wq_copy(2).start()
    wq_copy(3).start()

    def kvp(k):
        to = flip(k)
        return send(kvsend.at[to], kv.at[block_no], kvp_send.at[k - 1], kv_recv.at[block_no], at(to, z, c))

    def kv_arrival(block):
        return send(kv.at[block], kv.at[block], fwd_send.at[0], kv_recv.at[block], at(p, z, c))

    def along(k, act):
        from_ = flip(k)
        block = 4 * from_ + z
        for n, step in enumerate((1, -1)):
            ok = (z + step <= 3) if step > 0 else ((z + step >= 0) & (from_ < 3))

            @pl.when(ok)
            def _():
                act(send(kv.at[block], kv.at[block], kvz_send.at[2 * k + n], kv_recv.at[block], at(p, z + step, c)))

    def make_kv(i, _):
        j = px + i - 2 * px * i
        columns = pl.ds(pl.multiple_of(j * 2 * HEAD, 2 * HEAD), 2 * HEAD)
        k = _dot(a_s[...], w_s[0, :, columns])
        v = _dot(a_s[...], w_s[1, :, columns]).astype(jnp.bfloat16)
        for n in range(2):
            kvsend[2 * j + n, 0:ROWS, :] = turned(k[:, n * HEAD : (n + 1) * HEAD])
            flat = v[:, n * HEAD : (n + 1) * HEAD].T
            kvsend[2 * j + n, ROWS : ROWS + HEAD, :] = flat[:, :HEAD]
            kvsend[2 * j + n, ROWS + HEAD : 2 * ROWS, :] = flat[:, HEAD:]

        @pl.when(i == 0)
        def _():
            kv[block_no] = kvsend[p]
            kvp(1).start()
            along(0, lambda copy: copy.start())

    lax.fori_loop(0, 2, make_kv, None)
    kvp(2).start()
    kvp(3).start()

    def q_copy(i, to):
        return send(qsend.at[i], qall.at[p], q_send.at[i], q_recv.at[p], at(to, z, c))

    def make_q(i, _):
        wq_copy(i).wait()

        def part(j, _):
            columns = pl.ds(pl.multiple_of(j * 2 * HEAD, 2 * HEAD), 2 * HEAD)
            q = _dot(a_s[...], w_s[2 + i, :, columns])
            for n in range(2):
                qsend[i, 2 * j + n] = turned(q[:, n * HEAD : (n + 1) * HEAD])

        lax.fori_loop(0, 2, part, None)

        @pl.when(i < 3)
        def _():
            q_copy(i, flip(i + 1)).start()

        @pl.when(i > 0)
        def _():
            kv_arrival(4 * flip(i) + z).wait_recv()
            along(i, lambda copy: copy.start())

    lax.fori_loop(0, 4, make_q, None)
    qall[p] = qsend[3]
    for k in range(4):
        wo_start(k)

    def with_x(j, _):
        columns = pl.ds(pl.multiple_of((c * tiles + j) * WIDE, WIDE), WIDE)
        ysum[j] = xs[:, :, columns].reshape(ROWS, WIDE).astype(jnp.float32)

    lax.fori_loop(0, tiles, with_x, None)

    for b in range(4):
        top_s[b] = jnp.full((1, COLS), -jnp.inf, jnp.float32)
        acc_s[b] = jnp.zeros((HEAD + 8, COLS), jnp.float32)

    e = HEAD**-0.5 * LOG2E
    strips = range(0, COLS, STRIP)

    def block(b, j0, j1, masked):
        keys = jnp.concatenate([kv[j, 0:ROWS, :] for j in (j0, j1)], axis=0)
        q = qall[b].reshape(COLS, HEAD)
        flat = jnp.concatenate([kv[j, n : n + HEAD, :] for j in (j0, j1) for n in (ROWS, ROWS + HEAD)], axis=1)
        values = jnp.concatenate([flat, jnp.ones((8, 2 * ROWS), jnp.bfloat16)], axis=0)
        if masked:
            gap = (lax.rem(lax.broadcasted_iota(jnp.int32, (ROWS, STRIP), 1), ROWS)
                   - lax.broadcasted_iota(jnp.int32, (ROWS, STRIP), 0))
            ok = jnp.concatenate([gap >= (j - (4 * b + z)) * ROWS for j in (j0, j1)], axis=0)
        for n in strips:
            s = _dot(keys, q[n : n + STRIP, :], 1, 1)
            if masked:
                s = jnp.where(ok, s, -jnp.inf)
            old = top_s[b, :, n : n + STRIP]
            top = jnp.maximum(old, s.max(axis=0, keepdims=True))
            top_s[b, :, n : n + STRIP] = top
            w = jnp.exp2((s - top) * e).astype(jnp.bfloat16)
            acc_s[b, :, n : n + STRIP] = acc_s[b, :, n : n + STRIP] * jnp.exp2((old - top) * e) + _dot(values, w)

    def unit(t):
        g, k = lax.div(t, 4), lax.rem(t, 4)
        inner = jnp.where(z == 1, jnp.where(g < 2, 1 - g, g), jnp.where(g < 2, 2 - g, 9 - 3 * g))
        zz = jnp.where(middle, inner, jnp.where(z == 0, g, 3 - g))
        pp = flip(k)
        return pp, zz, 4 * pp + zz

    def forward(t, act):
        pp, zz, j = unit(t)
        for step, ok in ((1, (zz < z) & (z < 3)), (-1, (zz > z) & (z > 0) & (pp < 3))):
            @pl.when(ok)
            def _():
                act(send(kv.at[j], kv.at[j], fwd_send.at[j], kv_recv.at[j], at(p, z + step, c)))

    def arrive(t):
        pp, zz, j = unit(t)

        @pl.when((zz <= z) | (pp < 3))
        def _():
            kv_arrival(j).wait_recv()

        forward(t, lambda copy: copy.start())

    def visit(k, kq, base):
        pp, z0, j0 = unit(base + k)
        _, z1, j1 = unit(base + k + 4)
        b = flip(kq)

        @pl.when(pp < b)
        def _():
            block(b, j0, j1, False)

        @pl.when((pp == b) & ((z0 <= z) | (z1 <= z)))
        def _():
            block(b, j0, j1, True)

    def q_arrive(k):
        q_from = flip(k)
        send(qall.at[q_from], qall.at[q_from], q_send.at[0], q_recv.at[q_from], at(p, z, c)).wait_recv()

    def finish(b):
        total = acc_s[b, HEAD : HEAD + 1, :]
        return (acc_s[b, :HEAD, :] * (1 / total)).T.reshape(GROUP, ROWS, HEAD).astype(jnp.bfloat16)

    def o_copy(k):
        return send(osend.at[k - 1], oall.at[p, c], o_send.at[k - 1], o_recv.at[p, c], at(flip(k), z, c))

    def descending(i):
        b = 3 - i - jnp.where(3 - i <= p, 1, 0)
        bx, by = lax.div(b, 2), lax.rem(b, 2)
        return 2 * (px + bx - 2 * px * bx) + (py + by - 2 * py * by)

    def attend(s, _):
        far_s = s - 16
        by_keys = z == 3
        k = jnp.where(s < 16, lax.rem(s, 4), jnp.where(by_keys, lax.div(far_s, 3), lax.rem(s, 4)))
        kq = jnp.where(s < 16, lax.div(s, 4), jnp.where(by_keys, 1 + lax.rem(far_s + 15, 3), descending(lax.div(s, 4) - 4)))

        @pl.when(s < 4)
        def _():
            arrive(4 + s)

        @pl.when((s == 4) & middle)
        def _():
            lax.fori_loop(8, 12, lambda t, _: arrive(t), None)

        for n in (1, 2, 3):
            @pl.when(s == 4 * n)
            def _():
                q_arrive(n)

        @pl.when((s >= 16) & jnp.where(by_keys, kq == 1, s < 20))
        def _():
            @pl.when((z == 0) | (z == 3))
            def _():
                arrive(8 + k)

            arrive(12 + k)

        visit(k, kq, jnp.where(s < 16, 0, 8))

        @pl.when((s >= 16) & (k == 3))
        def _():
            osend[kq - 1] = finish(flip(kq))
            o_copy(kq).start()

    lax.fori_loop(0, 28, attend, None)
    lax.fori_loop(0, 4, lambda k, _: visit(k, 0, 8), None)

    def pass_on(k):
        g = flip(k)
        return send(oall.at[g, c], oall.at[g, c], p_send.at[k], o_recv.at[g, c], at(p, z, 1 - c))

    def o_arrive(k, core):
        g = flip(k)
        send(oall.at[g, core], oall.at[g, core], o_send.at[0], o_recv.at[g, core], at(p, z, c)).wait_recv()

    def heads(g, core):
        return jnp.concatenate([oall[g, core, n] for n in range(GROUP)], axis=1)

    oall[p, c] = finish(p)

    pass_on(0).start()

    def part(j, k, n):
        return w_s[k, pl.ds(pl.multiple_of((2 * j + n) * WIDE, WIDE), WIDE), :]

    def add(k, core, n):
        o = heads(flip(k), core)

        def tile(j, _):
            ysum[j] = ysum[j] + _dot(o, part(j, k, n))

        lax.fori_loop(0, tiles, tile, None)

    wo_wait(0)
    add(0, c, 0)

    def project(k, _):
        o_arrive(k, c)
        pass_on(k).start()
        wo_wait(k)
        o_arrive(k - 1, 1 - c)
        mine, theirs = heads(flip(k), c), heads(flip(k - 1), 1 - c)

        def tile(j, _):
            ysum[j] = ysum[j] + (_dot(mine, part(j, k, 0)) + _dot(theirs, part(j, k - 1, 1)))

        lax.fori_loop(0, tiles, tile, None)

    lax.fori_loop(1, 3, project, None)
    o_arrive(2, 1 - c)
    add(2, 1 - c, 1)
    o_arrive(3, c)
    pass_on(3).start()
    wo_wait(3)
    add(3, c, 0)
    o_arrive(3, 1 - c)
    other = heads(flip(3), 1 - c)

    def y_copy(j, core):
        columns = pl.ds(pl.multiple_of((core * tiles + j) * WIDE, WIDE), WIDE)
        return send(ysend.at[j], y_ref.at[:, columns], y_send.at[j], y_recv.at[j], at(p, z, 1 - c))

    def last(j, _):
        got = ysum[j] + _dot(other, part(j, 3, 1))
        got = got.astype(jnp.bfloat16)
        columns = pl.ds(pl.multiple_of((c * tiles + j) * WIDE, WIDE), WIDE)
        y_ref[:, columns] = jnp.where(c == 0, got[:OWN], got[OWN:])
        ysend[j] = jnp.where(c == 0, got[OWN:], got[:OWN])

        @pl.when(j > 0)
        def _():
            y_copy(j - 1, c).start()

    lax.fori_loop(0, tiles, last, None)
    y_copy(tiles - 1, c).start()
    lax.fori_loop(0, tiles, lambda j, _: y_copy(j, 1 - c).wait_recv(), None)

    for i in range(PIECES):
        x_piece(i, c).wait_send()
    for k in (1, 2, 3):
        kvp(k).wait_send()
        q_copy(k - 1, flip(k)).wait_send()
        o_copy(k).wait_send()
    for k in range(4):
        pass_on(k).wait_send()
    lax.fori_loop(0, tiles, lambda j, _: y_copy(j, c).wait_send(), None)

    def sent(k, _):
        along(k, lambda copy: copy.wait_send())

    lax.fori_loop(0, 4, sent, None)
    lax.fori_loop(4, BLOCKS, lambda t, _: forward(t, lambda copy: copy.wait_send()), None)


def tables():
    half = HEAD // 2
    speed = np.tile(float(THETA) ** (-np.arange(half) / half), 2)
    near, far = np.arange(ROWS)[:, None] * speed, ROWS * np.arange(BLOCKS)[:, None] * speed
    sign = np.broadcast_to(np.where(np.arange(HEAD) < half, -1.0, 1.0), far.shape)
    return np.stack([np.cos(near), np.sin(near)]).astype(np.float32), np.stack([np.cos(far), np.sin(far), sign]).astype(np.float32)


def layer(x, gain, wq, wk, wv, wo):
    dim = x.shape[1]
    tiles = dim // (2 * WIDE)
    bf16, f32 = jnp.bfloat16, jnp.float32
    dma = pltpu.SemaphoreType.DMA
    vmem = pl.BlockSpec(memory_space=pltpu.VMEM)
    hbm = pl.BlockSpec(memory_space=pl.ANY)
    near, far = tables()
    return pl.pallas_call(
        _kernel,
        out_shape=pltpu.VMEM(x.shape, bf16),
        in_specs=[hbm, vmem, hbm, hbm, hbm, hbm, hbm, hbm],
        out_specs=vmem,
        scratch_shapes=[
            pltpu.VMEM((2, OWN, dim), bf16),
            pltpu.VMEM((ROWS, dim), bf16),
            pltpu.VMEM((6, dim, WIDE), bf16),
            pltpu.VMEM(near.shape, f32),
            pltpu.VMEM(far.shape, f32),
            pltpu.VMEM((2, ROWS, HEAD), f32),
            pltpu.VMEM((4, 2 * ROWS, HEAD), bf16),
            pltpu.VMEM((BLOCKS, 2 * ROWS, HEAD), bf16),
            pltpu.VMEM((4, GROUP, ROWS, HEAD), bf16),
            pltpu.VMEM((4, GROUP, ROWS, HEAD), bf16),
            pltpu.VMEM((4, 1, COLS), f32),
            pltpu.VMEM((4, HEAD + 8, COLS), f32),
            pltpu.VMEM((3, GROUP, ROWS, HEAD), bf16),
            pltpu.VMEM((4, 2, GROUP, ROWS, HEAD), bf16),
            pltpu.VMEM((tiles, ROWS, WIDE), f32),
            pltpu.VMEM((tiles, OWN, WIDE), bf16),
            dma, dma((6,)), dma((4,)), dma((2,)), dma((PIECES,)), dma((PIECES,)), dma((3,)), dma((BLOCKS,)), dma((8,)), dma((BLOCKS,)),
            dma((3,)), dma((4,)), dma((3,)), dma((4, 2)), dma((4,)), dma((tiles,)), dma((tiles,)),
        ],
        compiler_params=pltpu.CompilerParams(collective_id=0, has_side_effects=True, vmem_limit_bytes=61 * 2**20),
        cost_estimate=pl.CostEstimate(flops=20 * 10**9, bytes_accessed=80 * 10**6, transcendentals=10**7),
    )(x, gain, jnp.asarray(near), jnp.asarray(far), wq, wk, wv, wo)


def solution(mesh):
    def step(x, gain, wq, wk, wv, wo):
        return layer(x, gain, wq, wk, wv, wo)

    tokens, whole = P(("dp", "sp"), None), P(None, None)
    return jax.shard_map(
        step,
        mesh=mesh,
        in_specs=(tokens, P(None), whole, whole, whole, whole),
        out_specs=tokens,
        check_vma=False,
    )
```
